32 devices in a mesh: year: 16 (over z, y, x), space: 2 (over core).
Axes of the slice: x: 2, y: 2, z: 4, core: 2. Of those that a mesh axis runs over, the one named last changes fastest.
Arguments:
- thermal_reading: float32 [2048, 8192], P('year', 'space'), may hold values from -24 to 24
- yearday_position: int32 [2048], P('year'), may hold values from 0 to 29, as said below
- usable_observation_tally: int32 [2048], P('year'), may hold values from 1 to 24
- location_surface_factor: float32 [8192], P('space'), may hold values from 0.2 to 5.4
Outputs:
- normalized_departure: float32 [2048, 8192], P('year', 'space')
- spread: float32 [2048], P('year')
The draws below stay inside these ranges and needn't reach their ends.
Inputs may be any that keep to these rules, and one draw needn't show every extreme that they name: `yearday_position`: every day of 0 to 29 is the day of at least one step.
All inputs are finite; a program needn't handle non-finite values.
Results may differ from the reference program's by a relative error of at most 0.0003.
Values sent between devices are 32-bit elements; how exact they have to be, the bound alone decides.
No kernel may reach another device: no remote copies, remote signals or barrier semaphores. Data moves between devices by JAX's collectives and lax.ppermute only.
A program may use at most 64 MiB of HBM per device.

```python
import jax
import jax.numpy as jnp
from jax import lax

DAYS = 30
NUM_DATES = 2048
NUM_LOCATIONS = 8192


def draw_yearday_position(key, part):
    first = jax.random.fold_in(key, 11)
    second = jax.random.fold_in(key, 12)
    days_drawn = jax.random.randint(first, (NUM_DATES,), 0, DAYS).astype(jnp.int32)
    places = jax.random.permutation(second, NUM_DATES)[:DAYS]
    return days_drawn.at[places].set(jnp.arange(DAYS, dtype=jnp.int32))


def draw_location_surface_factor(key, part):
    position = jnp.arange(NUM_LOCATIONS, dtype=jnp.float32)
    rising = 1.0 + 2.0 * position / max(NUM_LOCATIONS - 1, 1)
    jitter = jax.random.uniform(jax.random.fold_in(key, 22), (NUM_LOCATIONS,), jnp.float32, 0.6, 1.4)
    return (rising * jitter).astype(jnp.float32)


def set_ends(result, own_key, smallest, high):
    place = [jax.random.randint(jax.random.fold_in(own_key, axis), (), 0, length) for axis, length in enumerate(result.shape)]
    longest = result.shape.index(max(result.shape))
    next_to = place[:longest] + [(place[longest] + 1) % result.shape[longest]] + place[longest + 1:]
    return result.at[tuple(place)].set(smallest).at[tuple(next_to)].set(high)


def shard_levels(key, shape, shards, low, high):
    def one(dim, shards_of):
        draws = jax.random.uniform(jax.random.fold_in(jax.random.fold_in(key, 6), dim), (shards_of,), jnp.float32, low / len(shards), high / len(shards))
        return jnp.repeat(jnp.exp(draws), shape[dim] // shards_of).reshape((-1,) + (1,) * (len(shape) - dim - 1))

    gain = one(*shards[0])
    for cut in shards[1:]:
        gain = gain * one(*cut)
    return gain


def normal_values(key, extent, scale, limit, cuts=(), kind=jnp.bfloat16):
    values = jax.random.normal(key, extent, jnp.float32) * scale
    if len(cuts) > 0:
        values = shard_levels(key, extent, cuts, -0.22, 0.18) * values
    return jnp.clip(values, min=-limit, max=limit).astype(kind)


def setup_inputs(seed: int = 0) -> dict:
    key_of = jax.random.split(jax.random.key(seed), 5)
    return {
        "thermal_reading": normal_values(key_of[0], (NUM_DATES, NUM_LOCATIONS), 4.0, 24.0, ((0, 16), (1, 2)), jnp.float32),
        "yearday_position": draw_yearday_position(jax.random.fold_in(key_of[4], 71), 0),
        "usable_observation_tally": set_ends(jax.random.randint(key_of[2], (NUM_DATES,), 1, 25), jax.random.fold_in(key_of[2], 1), 1, 24).astype(jnp.int32),
        "location_surface_factor": draw_location_surface_factor(jax.random.fold_in(key_of[4], 71), 0),
    }


def reference(thermal_reading, yearday_position, usable_observation_tally, location_surface_factor):
    days_row = jnp.arange(DAYS, dtype=jnp.int32)
    yearday_onehot = (yearday_position[None, :] == days_row[:, None]).astype(jnp.float32)
    observation_tally = usable_observation_tally.astype(jnp.float32)
    surface_scaled_product = jnp.dot(yearday_onehot * observation_tally[None, :], thermal_reading, precision=lax.Precision.HIGHEST)
    hour_total = jnp.sum(yearday_onehot * observation_tally[None, :], axis=1)

    def extremes(which_day):
        picked_elements = (yearday_position == which_day)[:, None]
        ceiling_bound = jnp.max(jnp.where(picked_elements, thermal_reading, -jnp.inf), axis=0)
        bottom_bound = jnp.min(jnp.where(picked_elements, thermal_reading, jnp.inf), axis=0)
        return ceiling_bound, bottom_bound

    yearday_ceiling, yearday_floor = lax.map(extremes, days_row)
    day_mean = surface_scaled_product / hour_total[:, None]
    day_scale = 4.0 / (yearday_ceiling - yearday_floor + 1.0)
    dated_average = jnp.take(day_mean, yearday_position, axis=0)
    dated_deviation = jnp.take(day_scale, yearday_position, axis=0)
    normalized_departure = (thermal_reading - dated_average) * dated_deviation
    spread = jnp.sum(location_surface_factor[None, :] * normalized_departure * normalized_departure, axis=1) / jnp.sum(location_surface_factor)
    return normalized_departure, spread
```

```python
import functools

import jax
import jax.numpy as jnp
from jax import lax
from jax.experimental import pallas as pl
from jax.experimental.pallas import tpu as pltpu
from jax.sharding import PartitionSpec as P

DAYS = 30
SUBLANES, LANES = 8, 128
GROUPS = 4
SLOTS = -(-DAYS // GROUPS)
CHUNKS = 2
HALVINGS = 3
HOURS, HIGH, LOW, TILES = SLOTS, SLOTS + 1, 2 * SLOTS + 1, 3 * SLOTS + 1
ORDERS = (((0, 1), (1, 0), (2, 2), (3, 3)), ((2, 2), (1, 0), (0, 1), (3, 3)))
AXES = ("year", "space")


def stage_bits(chunk, years):
    count = years.bit_length() - 1
    assert years == 1 << count and count > HALVINGS
    return [tuple(1 << b for b in pair) for pair in ORDERS[chunk]] + [(1 << b, 1 << b) for b in range(4, count)]


def own_bits(chunk):
    year, core = lax.axis_index("year"), lax.rem(lax.axis_index("space"), 2)
    pairs = stage_bits(chunk, lax.axis_size("year"))[:HALVINGS]
    return [jnp.where(core == 0, year // a % 2, year // b % 2) for a, b in pairs]


def place(day, bits):
    group, index = day // SLOTS, day % SLOTS
    second = 1 - (group // 2 + bits[1]) % 2
    third = 1 - (group % 2 + bits[2]) % 2
    return second, third, index


def stats_kernel(chunk, day_ref, tally_ref, x_ref, out_ref):
    bits = own_bits(chunk)
    tiles, rows = x_ref.shape[0], x_ref.shape[1] // 2
    height = rows // SUBLANES
    for half in range(2):
        for second in range(2):
            for third in range(2):
                block = out_ref.at[half, second, third]
                block[:HIGH] = jnp.zeros((HIGH, height, LANES), jnp.float32)
                block[HIGH:] = jnp.full((TILES - HIGH, height, LANES), -jnp.inf, jnp.float32)
    starts = [(1 - bits[0]) * rows, bits[0] * rows]

    def tile(t, carry):
        for k in range(SUBLANES):
            step = t * SUBLANES + k
            second, third, index = place(day_ref[step], bits)
            tally = tally_ref[step].astype(jnp.float32)
            for half in range(2):
                x = x_ref[t, pl.ds(starts[half] + k, height, stride=SUBLANES), :]
                out = out_ref.at[half, second, third]
                out[index] += tally * x
                out[HIGH + index] = jnp.maximum(out[HIGH + index], x)
                out[LOW + index] = jnp.maximum(out[LOW + index], -x)
                out[HOURS, pl.ds(index, 1), :] += jnp.full((1, LANES), tally, jnp.float32)
        return carry

    lax.fori_loop(0, tiles, tile, 0)


def stats(chunk, day, tally, x):
    tiles, rows = x.shape[0], x.shape[1] // CHUNKS
    shape = (2, 2, 2, TILES, rows // 2 // SUBLANES, LANES)
    return pl.pallas_call(
        functools.partial(stats_kernel, chunk),
        grid=(1,),
        in_specs=[
            pl.BlockSpec(memory_space=pltpu.SMEM),
            pl.BlockSpec(memory_space=pltpu.SMEM),
            pl.BlockSpec((tiles, rows, LANES), lambda i: (0, chunk, 0)),
        ],
        out_specs=pl.BlockSpec(shape, lambda i: (0,) * 6),
        out_shape=jax.ShapeDtypeStruct(shape, jnp.float32),
        name=f"stats_{chunk}",
    )(day, tally, x)


def depart_kernel(chunk, day_ref, x_ref, w_ref, recv_ref, own_ref, before_ref, *rest):
    out_ref, sums_ref, squares = rest[-3:]
    bits = own_bits(chunk)
    tiles, rows = x_ref.shape[0], x_ref.shape[1] // 2
    height = rows // SUBLANES
    starts = [(1 - bits[0]) * rows, bits[0] * rows]
    weights = [w_ref[pl.ds(pl.multiple_of((chunk * 2 + b) * height, height), height), :] for b in (1 - bits[0], bits[0])]

    def tile(t, carry):
        for k in range(SUBLANES):
            second, third, index = place(day_ref[t * SUBLANES + k], bits)
            total = None
            for half, table_ref in enumerate((recv_ref, own_ref)):
                place_x = pl.ds(starts[half] + k, height, stride=SUBLANES)
                table = table_ref.at[second, third]
                departure = (x_ref[t, place_x, :] - table[index]) * table[SLOTS + index]
                out_ref[t, place_x, :] = departure
                square = weights[half] * departure * departure
                total = square if total is None else total + square
            squares[pl.ds(pl.multiple_of((t * SUBLANES + k) * height, height), height), :] = total
        return carry

    lax.fori_loop(0, tiles, tile, 0)

    def fold(t, carry):
        start = t * SUBLANES * height
        total = squares[pl.ds(start, SUBLANES, stride=height), :]
        for j in range(1, height):
            total += squares[pl.ds(start + j, SUBLANES, stride=height), :]
        here = pl.ds(pl.multiple_of(t * SUBLANES, SUBLANES), SUBLANES)
        sums_ref[here, :] = total if before_ref is None else total + before_ref[here, :]
        return carry

    lax.fori_loop(0, tiles, fold, 0)


def depart(chunk, day, x, w, recv, own, before, out):
    tiles, rows = x.shape[0], x.shape[1] // CHUNKS
    height = rows // 2 // SUBLANES
    whole = lambda a: pl.BlockSpec(a.shape, lambda i, n=a.ndim: (0,) * n)
    column = pl.BlockSpec((tiles, rows, LANES), lambda i: (0, chunk, 0))
    steps = tiles * SUBLANES
    kernel = functools.partial(depart_kernel, chunk)
    inputs = [day, x, w, recv, own]
    in_specs = [pl.BlockSpec(memory_space=pltpu.SMEM), column, whole(w), whole(recv), whole(own)]
    aliases = {}
    if out is None:
        kernel = lambda *refs: depart_kernel(chunk, *refs[:5], None, *refs[5:])
    else:
        inputs += [before, out]
        in_specs += [whole(before), pl.BlockSpec(memory_space=pl.ANY)]
        aliases = {6: 0}
    return pl.pallas_call(
        kernel,
        grid=(1,),
        in_specs=in_specs,
        out_specs=(column, pl.BlockSpec((steps, LANES), lambda i: (0, 0))),
        out_shape=(jax.ShapeDtypeStruct(x.shape, jnp.float32), jax.ShapeDtypeStruct((steps, LANES), jnp.float32)),
        scratch_shapes=[pltpu.VMEM((steps * height, LANES), jnp.float32)],
        input_output_aliases=aliases,
        name=f"depart_{chunk}",
    )(*inputs)


def merge(a, b):
    adds = lax.broadcasted_iota(jnp.int32, (TILES, 1, 1), 0) < HIGH
    return jnp.where(adds, a + b, jnp.maximum(a, b))


def exchange(x, pair):
    years, spaces = lax.axis_size("year"), lax.axis_size("space")
    partners = [(y * spaces + s, (y ^ pair[s % 2]) * spaces + s) for y in range(years) for s in range(spaces)]
    return lax.ppermute(x, AXES, partners)


def day_tables(chunk, local):
    pairs = stage_bits(chunk, lax.axis_size("year"))
    send, keep = local[0], local[1]
    for stage, pair in enumerate(pairs):
        got = exchange(send if stage < HALVINGS else keep, pair)
        yield
        if stage < HALVINGS - 1:
            send, keep = merge(got[0], keep[0]), merge(got[1], keep[1])
        else:
            keep = merge(got, keep)
    mean = keep[:SLOTS] / keep[HOURS][:, None, :]
    scale = 4.0 / (keep[HIGH:LOW] + keep[LOW:] + 1.0)
    table = jnp.concatenate([mean, scale])
    for stage in reversed(range(HALVINGS)):
        got = exchange(table, pairs[stage])
        yield
        if stage > 0:
            table = jnp.stack([got, table])
    yield got, table


def on_device(thermal_reading, yearday_position, usable_observation_tally, location_surface_factor):
    steps, cells = thermal_reading.shape
    tiles, columns = steps // SUBLANES, cells // LANES
    x = thermal_reading.reshape(tiles, SUBLANES, columns, LANES).transpose(0, 2, 1, 3)
    x = x.reshape(tiles, columns * SUBLANES, LANES)
    w = location_surface_factor.reshape(columns, LANES)
    chunks = [day_tables(c, stats(c, yearday_position, usable_observation_tally, x)) for c in range(CHUNKS)]
    results = [None] * CHUNKS
    while not all(results):
        for c in range(CHUNKS):
            results[c] = next(chunks[c])
    out = sums = None
    for c in range(CHUNKS):
        out, sums = depart(c, yearday_position, x, w, *results[c], sums, out)
    weighted_sq, area_total = jnp.sum(sums, axis=1), jnp.sum(location_surface_factor)
    weighted_sq, area_total = lax.psum((weighted_sq, area_total), "space")
    out = out.reshape(tiles, columns, SUBLANES, LANES).transpose(0, 2, 1, 3).reshape(steps, cells)
    return out, weighted_sq / area_total


def solution(mesh):
    return jax.shard_map(
        on_device,
        mesh=mesh,
        in_specs=(P("year", "space"), P("year"), P("year"), P("space")),
        out_specs=(P("year", "space"), P("year")),
        check_vma=False,
    )
```

```python
import functools

import jax
import jax.numpy as jnp
from jax import lax
from jax.experimental import pallas as pl
from jax.experimental.pallas import tpu as pltpu
from jax.sharding import PartitionSpec as P

DAYS = 30
SUBLANES, LANES = 8, 128
GROUPS = 4
SLOTS = -(-DAYS // GROUPS)
CHUNKS = 2
HALVINGS = 3
HOURS, HIGH, LOW, TILES = SLOTS, SLOTS + 1, 2 * SLOTS + 1, 3 * SLOTS + 1
ORDERS = (((0, 1), (1, 0), (2, 2), (3, 3)), ((2, 2), (1, 0), (0, 1), (3, 3)))
AXES = ("year", "space")
PIECES = 4

VMEM = pl.BlockSpec(memory_space=pltpu.VMEM)
SMEM = pl.BlockSpec(memory_space=pltpu.SMEM)
HBM = pl.BlockSpec(memory_space=pltpu.HBM)


def local_call(kernel, name, out_shape, *inputs, **options):
    specs = options.pop("in_specs", [VMEM] * len(inputs))
    spaces = {id(VMEM): pltpu.VMEM, id(HBM): pltpu.HBM}
    inputs = [pltpu.with_memory_space_constraint(a, spaces[id(s)]) if id(s) in spaces else a for a, s in zip(inputs, specs)]
    limit = pltpu.CompilerParams(vmem_limit_bytes=options.pop("vmem", 1 << 20))
    return pl.pallas_call(kernel, in_specs=specs, out_shape=out_shape, name=name, compiler_params=limit, **options)(*inputs)


def vmem(*shape):
    return pltpu.VMEM(shape, jnp.float32)


def stage_bits(chunk, years):
    count = years.bit_length() - 1
    assert years == 1 << count and count > HALVINGS
    return [tuple(1 << b for b in pair) for pair in ORDERS[chunk]] + [(1 << b, 1 << b) for b in range(4, count)]


def own_bits(chunk):
    year, core = lax.axis_index("year"), lax.rem(lax.axis_index("space"), 2)
    pairs = stage_bits(chunk, lax.axis_size("year"))[:HALVINGS]
    return [jnp.where(core == 0, year // a % 2, year // b % 2) for a, b in pairs]


def day_flip(bits):
    return ((1 - bits[1]) * 2 + 1 - bits[2]) * SLOTS


def place(day, flip):
    day = lax.bitwise_xor(day, flip)
    return lax.shift_right_logical(day, SLOTS.bit_length() - 1), lax.bitwise_and(day, SLOTS - 1)


def stats_kernel(chunk, *refs):
    if chunk == 0:
        day_in, tally_in, x_in, send_ref, keep_ref, x_ref, day_ref, tally_ref, hours, arrived, listed = refs
        tiles, rows = x_in.shape[0], x_in.shape[1] // CHUNKS
        piece = tiles // PIECES
        lists = [pltpu.make_async_copy(day_in, day_ref, listed.at[0]), pltpu.make_async_copy(tally_in, tally_ref, listed.at[1])]
        copies = []
        for c in range(CHUNKS):
            for p in range(PIECES):
                at = pl.ds(p * piece, piece), pl.ds(c * rows, rows)
                copies.append(pltpu.make_async_copy(x_in.at[at], x_ref.at[at], arrived.at[c, p]))
        for copy in lists + copies:
            copy.start()
    else:
        day_ref, tally_ref, x_ref, send_ref, keep_ref, hours = refs
        tiles, rows = x_ref.shape[0], x_ref.shape[1] // CHUNKS
        piece, lists, copies = tiles // PIECES, [], []
    bits = own_bits(chunk)
    flip = day_flip(bits)
    half = rows // 2
    height = half // SUBLANES
    outs = [ref.reshape(GROUPS, *ref.shape[2:]) for ref in (send_ref, keep_ref)]
    starts = [chunk * rows + (1 - bits[0]) * half, chunk * rows + bits[0] * half]
    for out in outs:
        for slot in range(GROUPS):
            block = out.at[slot]
            block[:HIGH] = jnp.zeros((HIGH, height, LANES), jnp.float32)
            block[HIGH:LOW] = jnp.full((SLOTS, height, LANES), -jnp.inf, jnp.float32)
            block[LOW:] = jnp.full((SLOTS, height, LANES), jnp.inf, jnp.float32)
    for d in range(GROUPS * SLOTS):
        hours[d] = 0
    for copy in lists:
        copy.wait()

    def tile(t, carry):
        for k in range(SUBLANES):
            step = t * SUBLANES + k
            day, tally = day_ref[step], tally_ref[step]
            slot, index = place(day, flip)
            hours[day] += tally
            tally = tally.astype(jnp.float32)
            blocks = [out.at[slot] for out in outs]
            x = [x_ref[t, pl.ds(start + k, height, stride=SUBLANES), :] for start in starts]
            old = [[b[index], b[HIGH + index], b[LOW + index]] for b in blocks]
            new = [[o[0] + tally * v, jnp.maximum(o[1], v), jnp.minimum(o[2], v)] for o, v in zip(old, x)]
            for b, n in zip(blocks, new):
                b[index], b[HIGH + index], b[LOW + index] = n
        return carry

    for p in range(PIECES):
        if copies:
            copies[p].wait()
        lax.fori_loop(p * piece, (p + 1) * piece, tile, 0)
    for d in range(DAYS):
        slot, index = place(jnp.int32(d), flip)
        row = jnp.full((1, LANES), hours[d].astype(jnp.float32), jnp.float32)
        for out in outs:
            out[slot, HOURS, pl.ds(index, 1), :] = row
    for copy in copies[PIECES:]:
        copy.wait()


def stats(chunk, day, tally, x):
    tiles, rows = x.shape[0], x.shape[1] // CHUNKS
    half = vmem(2, GROUPS // 2, TILES, rows // 2 // SUBLANES, LANES)
    shapes, scratch = (half, half), [pltpu.SMEM((GROUPS * SLOTS,), jnp.int32)]
    if chunk == 0:
        shapes += (vmem(*x.shape),)
        lists = [pltpu.SMEM(day.shape, jnp.int32)] * 2
        scratch = lists + scratch + [pltpu.SemaphoreType.DMA((CHUNKS, PIECES)), pltpu.SemaphoreType.DMA((2,))]
    return local_call(
        functools.partial(stats_kernel, chunk),
        f"stats_{chunk}",
        shapes,
        day, tally, x,
        in_specs=[HBM] * 3 if chunk == 0 else [SMEM, SMEM, VMEM],
        out_specs=(VMEM,) * len(shapes),
        scratch_shapes=scratch,
    )


def split_kernel(got_ref, own_ref, *outs):
    lead = got_ref.shape[:-3]
    for i in range(got_ref.size // got_ref.shape[-1] // got_ref.shape[-2] // TILES):
        at, rest = [], i
        for n in reversed(lead):
            at.insert(0, rest % n)
            rest //= n
        out = outs[at[0]] if len(outs) > 1 else outs[0]
        for a, b, join in ((0, HIGH, jnp.add), (HIGH, LOW, jnp.maximum), (LOW, TILES, jnp.minimum)):
            value = join(got_ref.at[tuple(at)][a:b], own_ref.at[tuple(at)][a:b])
            (out.at[tuple(at[1:])] if len(at) > 1 else out)[a:b] = value


def table_kernel(got_ref, own_ref, table_ref):
    height = got_ref.shape[1]
    hours = got_ref[HOURS] + own_ref[HOURS]
    for i in range(SLOTS):
        total = got_ref[i] + own_ref[i]
        table_ref[i] = total / jnp.broadcast_to(hours[i : i + 1], (height, LANES))
        high = jnp.maximum(got_ref[HIGH + i], own_ref[HIGH + i])
        low = jnp.minimum(got_ref[LOW + i], own_ref[LOW + i])
        table_ref[SLOTS + i] = 4.0 / (high - low + 1.0)


def join_kernel(got_ref, own_ref, out_ref):
    out_ref[0] = got_ref[...]
    out_ref[1] = own_ref[...]


def depart_kernel(chunk, last, day_ref, x_ref, w_ref, recv_ref, own_ref, *refs):
    if chunk > 0:
        before_ref, refs = refs[0], refs[2:]
    out_ref, sums_ref, squares, ready, left = refs
    tiles, rows = x_ref.shape[0], x_ref.shape[1] // CHUNKS
    piece = tiles // PIECES
    bits = own_bits(chunk)
    flip = day_flip(bits)
    tables = [ref.reshape(GROUPS, *ref.shape[2:]) for ref in (recv_ref, own_ref)]
    half_rows = rows // 2
    height = half_rows // SUBLANES
    starts = [(1 - bits[0]) * half_rows, bits[0] * half_rows]
    weights = [w_ref[pl.ds(pl.multiple_of((chunk * 2 + b) * height, height), height), :] for b in (1 - bits[0], bits[0])]

    def tile(t, carry):
        for k in range(SUBLANES):
            slot, index = place(day_ref[t * SUBLANES + k], flip)
            total = None
            for half, table_ref in enumerate(tables):
                at = pl.ds(chunk * rows + starts[half] + k, height, stride=SUBLANES)
                table = table_ref.at[slot]
                departure = (x_ref[t, at, :] - table[index]) * table[SLOTS + index]
                ready[t, pl.ds(starts[half] + k, height, stride=SUBLANES), :] = departure
                square = weights[half] * departure * departure
                total = square if total is None else total + square
            squares[pl.ds(pl.multiple_of((t * SUBLANES + k) * height, height), height), :] = total
        return carry

    copies = []
    for p in range(PIECES):
        lax.fori_loop(p * piece, (p + 1) * piece, tile, 0)
        at = pl.ds(p * piece, piece)
        copies.append(pltpu.make_async_copy(ready.at[at], out_ref.at[at, pl.ds(chunk * rows, rows)], left.at[p]))
        copies[-1].start()
    sums = []
    for t in range(tiles):
        start = t * SUBLANES * height
        total = squares[pl.ds(start, SUBLANES, stride=height), :]
        for j in range(1, height):
            total += squares[pl.ds(start + j, SUBLANES, stride=height), :]
        at = pl.ds(t * SUBLANES, SUBLANES)
        if chunk > 0:
            total += before_ref[at, :]
        if last:
            sums.append(total)
        else:
            sums_ref[at, :] = total
    if last:
        by_step = jnp.sum(jnp.concatenate(sums).T, axis=0, keepdims=True)
        sums_ref[0:1, :] = by_step
        sums_ref[1:2, :] = jnp.full(by_step.shape, jnp.sum(w_ref[...]), jnp.float32)
        sums_ref[2:, :] = jnp.zeros((SUBLANES - 2, by_step.shape[1]), jnp.float32)
    for copy in copies:
        copy.wait()


def depart(chunk, day, x, w, recv, own, before, out):
    tiles, rows = x.shape[0], x.shape[1] // CHUNKS
    steps, last = tiles * SUBLANES, chunk == CHUNKS - 1
    inputs, specs, aliases = [day, x, w, recv, own], [SMEM] + [VMEM] * 4, {}
    if chunk > 0:
        inputs, specs, aliases = inputs + [before, out], specs + [VMEM, HBM], {6: 0}
    return local_call(
        functools.partial(depart_kernel, chunk, last),
        f"depart_{chunk}",
        (pltpu.HBM((tiles, rows * CHUNKS, LANES), jnp.float32), vmem(SUBLANES if last else steps, steps if last else LANES)),
        *inputs,
        in_specs=specs,
        out_specs=(HBM, VMEM),
        scratch_shapes=[
            pltpu.VMEM((rows // 2 * tiles, LANES), jnp.float32),
            pltpu.VMEM((tiles, rows, LANES), jnp.float32),
            pltpu.SemaphoreType.DMA((PIECES,)),
        ],
        input_output_aliases=aliases,
        vmem=4 << 20,
    )


def exchange(x, pair, name):
    years, spaces = lax.axis_size("year"), lax.axis_size("space")
    partners = [(y * spaces + s, (y ^ pair[s % 2]) * spaces + s) for y in range(years) for s in range(spaces)]
    with jax.named_scope(name):
        return lax.ppermute(pltpu.with_memory_space_constraint(x, pltpu.VMEM), AXES, partners)


def day_tables(chunk, send, keep):
    pairs = stage_bits(chunk, lax.axis_size("year"))
    for stage, pair in enumerate(pairs):
        got = exchange(send if stage < HALVINGS else keep, pair, f"send_{chunk}_{stage}")
        yield
        name = f"merge_{chunk}_{stage}"
        if stage < HALVINGS - 1:
            half = vmem(*got.shape[1:])
            send, keep = local_call(split_kernel, name, (half, half), got, keep, out_specs=(VMEM, VMEM))
        elif stage < len(pairs) - 1:
            keep = local_call(split_kernel, name, vmem(*got.shape), got, keep, out_specs=VMEM)
    table = local_call(table_kernel, name, vmem(2 * SLOTS, *got.shape[1:]), got, keep, out_specs=VMEM)
    for stage in reversed(range(HALVINGS)):
        number = len(pairs) + HALVINGS - 1 - stage
        got = exchange(table, pairs[stage], f"send_{chunk}_{number}")
        yield
        if stage > 0:
            table = local_call(join_kernel, f"merge_{chunk}_{number}", vmem(2, *got.shape), got, table, out_specs=VMEM)
    yield got, table


def on_device(thermal_reading, yearday_position, usable_observation_tally, location_surface_factor):
    steps, cells = thermal_reading.shape
    tiles, columns = steps // SUBLANES, cells // LANES
    x = thermal_reading.reshape(tiles, SUBLANES, columns, LANES).transpose(0, 2, 1, 3)
    x = x.reshape(tiles, columns * SUBLANES, LANES)
    w = location_surface_factor.reshape(columns, LANES)
    chunks = []
    for c in range(CHUNKS):
        send, keep, *copied = stats(c, yearday_position, usable_observation_tally, x)
        if copied:
            x = copied[0]
        chunks.append(day_tables(c, send, keep))
    results = [None] * CHUNKS
    while not all(results):
        for c in range(CHUNKS):
            results[c] = next(chunks[c])
    out = sums = None
    for c in range(CHUNKS):
        out, sums = depart(c, yearday_position, x, w, *results[c], sums, out)
    if lax.axis_size("space") == 2:
        sums += lax.ppermute(sums, "space", [(0, 1), (1, 0)])
    else:
        sums = lax.psum(sums, "space")
    out = out.reshape(tiles, columns, SUBLANES, LANES).transpose(0, 2, 1, 3).reshape(steps, cells)
    return out, sums[0] / sums[1]


def solution(mesh):
    return jax.shard_map(
        on_device,
        mesh=mesh,
        in_specs=(P("year", "space"), P("year"), P("year"), P("space")),
        out_specs=(P("year", "space"), P("year")),
        check_vma=False,
    )
```

```python
import functools
import math

import jax
import jax.numpy as jnp
from jax import lax
from jax.experimental import pallas as pl
from jax.experimental.pallas import tpu as pltpu
from jax.sharding import PartitionSpec as P

DAYS = 30
SUBLANES, LANES = 8, 128
GROUPS = 2
SLOTS = -(-DAYS // GROUPS)
CHUNKS = 2
HALVINGS = 2
REST = 2 * GROUPS >> HALVINGS
HOURS, HIGH, LOW, TILES = SLOTS, SLOTS + 1, 2 * SLOTS + 1, 3 * SLOTS + 1
ORDERS = (((0, 2), (1, 3), (2, 1), (3, 0)), ((1, 2), (0, 3), (3, 1), (2, 0)))
AXES = ("year", "space")
PIECES = 4

VMEM = pl.BlockSpec(memory_space=pltpu.VMEM)
SMEM = pl.BlockSpec(memory_space=pltpu.SMEM)
HBM = pl.BlockSpec(memory_space=pltpu.HBM)


def local_call(kernel, name, out_shape, *inputs, **options):
    specs = options.pop("in_specs", [VMEM] * len(inputs))
    spaces = {id(VMEM): pltpu.VMEM, id(HBM): pltpu.HBM}
    inputs = [pltpu.with_memory_space_constraint(a, spaces[id(s)]) if id(s) in spaces else a for a, s in zip(inputs, specs)]
    limit = pltpu.CompilerParams(vmem_limit_bytes=options.pop("vmem", 1 << 20))
    return pl.pallas_call(kernel, in_specs=specs, out_shape=out_shape, name=name, compiler_params=limit, **options)(*inputs)


def vmem(*shape):
    return pltpu.VMEM(shape, jnp.float32)


def stage_bits(chunk, years):
    assert HALVINGS > 1 and 2 * GROUPS >= 1 << HALVINGS and SLOTS <= 2 * SUBLANES
    count = years.bit_length() - 1
    assert years == 1 << count and count > HALVINGS
    return [tuple(1 << b for b in pair) for pair in ORDERS[chunk]] + [(1 << b, 1 << b) for b in range(4, count)]


def own_bits(chunk):
    year, core = lax.axis_index("year"), lax.rem(lax.axis_index("space"), 2)
    pairs = stage_bits(chunk, lax.axis_size("year"))[:HALVINGS]
    return [jnp.where(core == 0, year // a % 2, year // b % 2) for a, b in pairs]


def day_flip(bits):
    return sum((1 - bit) * (GROUPS >> i) for i, bit in enumerate(bits) if i > 0)


def place(day, flip):
    group = sum((day >= g * SLOTS).astype(jnp.int32) for g in range(1, GROUPS))
    return lax.bitwise_xor(group, flip), day - group * SLOTS


def by_group(*refs):
    return [ref.reshape(math.prod(ref.shape[:-3]), *ref.shape[-3:]) if len(ref.shape) > 3 else ref for ref in refs]


def stats_kernel(chunk, *refs):
    if chunk == 0:
        day_in, tally_in, x_in, send_ref, keep_ref, x_ref, day_ref, tally_ref, hours, arrived, listed = refs
        tiles, rows = x_in.shape[0], x_in.shape[1] // CHUNKS
        piece = tiles // PIECES
        lists = [pltpu.make_async_copy(day_in, day_ref, listed.at[0]), pltpu.make_async_copy(tally_in, tally_ref, listed.at[1])]
        copies = []
        for c in range(CHUNKS):
            for p in range(PIECES):
                at = pl.ds(p * piece, piece), pl.ds(c * rows, rows)
                copies.append(pltpu.make_async_copy(x_in.at[at], x_ref.at[at], arrived.at[c, p]))
        for copy in lists + copies:
            copy.start()
    else:
        day_ref, tally_ref, x_ref, send_ref, keep_ref, hours = refs
        tiles, rows = x_ref.shape[0], x_ref.shape[1] // CHUNKS
        piece, lists, copies = tiles // PIECES, [], []
    bits = own_bits(chunk)
    flip = day_flip(bits)
    half = rows // 2
    height = half // SUBLANES
    outs = by_group(send_ref, keep_ref)
    starts = [chunk * rows + (1 - bits[0]) * half, chunk * rows + bits[0] * half]
    for out in outs:
        for slot in range(GROUPS):
            block = out.at[slot]
            block[:HIGH] = jnp.zeros((HIGH, height, LANES), jnp.float32)
            block[HIGH:LOW] = jnp.full((SLOTS, height, LANES), -jnp.inf, jnp.float32)
            block[LOW:] = jnp.full((SLOTS, height, LANES), jnp.inf, jnp.float32)
    for d in range(GROUPS * SLOTS):
        hours[d] = 0
    for copy in lists:
        copy.wait()

    def tile(t, carry):
        for k in range(SUBLANES):
            step = t * SUBLANES + k
            day, tally = day_ref[step], tally_ref[step]
            slot, index = place(day, flip)
            hours[day] += tally
            tally = tally.astype(jnp.float32)
            blocks = [out.at[slot] for out in outs]
            x = [x_ref[t, pl.ds(start + k, height, stride=SUBLANES), :] for start in starts]
            old = [[b[index], b[HIGH + index], b[LOW + index]] for b in blocks]
            new = [[o[0] + tally * v, jnp.maximum(o[1], v), jnp.minimum(o[2], v)] for o, v in zip(old, x)]
            for b, n in zip(blocks, new):
                b[index], b[HIGH + index], b[LOW + index] = n
        return carry

    for p in range(PIECES):
        if copies:
            copies[p].wait()
        lax.fori_loop(p * piece, (p + 1) * piece, tile, 0)
    left = lax.broadcasted_iota(jnp.int32, (1, LANES), 1) < LANES // 2
    for group in range(GROUPS):
        slot = lax.bitwise_xor(group, flip)
        for k in range(SUBLANES):
            pair = [hours[group * SLOTS + min(i, SLOTS - 1)].astype(jnp.float32) for i in (k, k + SUBLANES)]
            for out in outs:
                out[slot, HOURS, k : k + 1, :] = jnp.where(left, *pair)
    for copy in copies[PIECES:]:
        copy.wait()


def stats(chunk, day, tally, x):
    tiles, rows = x.shape[0], x.shape[1] // CHUNKS
    half = vmem(*(2,) * (HALVINGS - 1), REST, TILES, rows // 2 // SUBLANES, LANES)
    shapes, scratch = (half, half), [pltpu.SMEM((GROUPS * SLOTS,), jnp.int32)]
    if chunk == 0:
        shapes += (vmem(*x.shape),)
        lists = [pltpu.SMEM(day.shape, jnp.int32)] * 2
        scratch = lists + scratch + [pltpu.SemaphoreType.DMA((CHUNKS, PIECES)), pltpu.SemaphoreType.DMA((2,))]
    return local_call(
        functools.partial(stats_kernel, chunk),
        f"stats_{chunk}",
        shapes,
        day, tally, x,
        in_specs=[HBM] * 3 if chunk == 0 else [SMEM, SMEM, VMEM],
        out_specs=(VMEM,) * len(shapes),
        scratch_shapes=scratch,
    )


def merge_kernel(got_ref, own_ref, *out_refs):
    got, own, *outs = by_group(got_ref, own_ref, *out_refs)
    each = got.shape[0] // len(outs)
    for i in range(got.shape[0]):
        for a, b, join in ((0, HIGH, jnp.add), (HIGH, LOW, jnp.maximum), (LOW, TILES, jnp.minimum)):
            outs[i // each][i % each, a:b] = join(got[i, a:b], own[i, a:b])


def table_kernel(got_ref, own_ref, table_ref):
    for g in range(REST):
        got, own, table = got_ref.at[g], own_ref.at[g], table_ref.at[g]
        hours = got[HOURS] + own[HOURS]
        left = lax.broadcasted_iota(jnp.int32, hours.shape, 1) < LANES // 2
        other = pltpu.roll(hours, LANES // 2, axis=1)
        hours = jnp.concatenate([jnp.where(left, hours, other), jnp.where(left, other, hours)])
        for i in range(SLOTS):
            total = got[i] + own[i]
            table[i] = total / jnp.broadcast_to(hours[i : i + 1], total.shape)
            high = jnp.maximum(got[HIGH + i], own[HIGH + i])
            low = jnp.minimum(got[LOW + i], own[LOW + i])
            table[SLOTS + i] = 4.0 / (high - low + 1.0)


def join_kernel(got_ref, own_ref, out_ref):
    out_ref[0] = got_ref[...]
    out_ref[1] = own_ref[...]


def depart_kernel(chunk, last, day_ref, x_ref, w_ref, recv_ref, own_ref, *refs):
    if chunk > 0:
        before_ref, refs = refs[0], refs[2:]
    out_ref, sums_ref, squares, ready, left = refs
    tiles, rows = x_ref.shape[0], x_ref.shape[1] // CHUNKS
    piece = tiles // PIECES
    bits = own_bits(chunk)
    flip = day_flip(bits)
    tables = by_group(recv_ref, own_ref)
    half_rows = rows // 2
    height = half_rows // SUBLANES
    starts = [(1 - bits[0]) * half_rows, bits[0] * half_rows]
    weights = [w_ref[pl.ds(pl.multiple_of((chunk * 2 + b) * height, height), height), :] for b in (1 - bits[0], bits[0])]

    def tile(t, carry):
        for k in range(SUBLANES):
            slot, index = place(day_ref[t * SUBLANES + k], flip)
            total = None
            for half, table_ref in enumerate(tables):
                at = pl.ds(chunk * rows + starts[half] + k, height, stride=SUBLANES)
                table = table_ref.at[slot]
                departure = (x_ref[t, at, :] - table[index]) * table[SLOTS + index]
                ready[t, pl.ds(starts[half] + k, height, stride=SUBLANES), :] = departure
                square = weights[half] * departure * departure
                total = square if total is None else total + square
            squares[pl.ds(pl.multiple_of((t * SUBLANES + k) * height, height), height), :] = total
        return carry

    copies = []
    for p in range(PIECES):
        lax.fori_loop(p * piece, (p + 1) * piece, tile, 0)
        at = pl.ds(p * piece, piece)
        copies.append(pltpu.make_async_copy(ready.at[at], out_ref.at[at, pl.ds(chunk * rows, rows)], left.at[p]))
        copies[-1].start()
    sums = []
    for t in range(tiles):
        start = t * SUBLANES * height
        total = squares[pl.ds(start, SUBLANES, stride=height), :]
        for j in range(1, height):
            total += squares[pl.ds(start + j, SUBLANES, stride=height), :]
        at = pl.ds(t * SUBLANES, SUBLANES)
        if chunk > 0:
            total += before_ref[at, :]
        if last:
            sums.append(total)
        else:
            sums_ref[at, :] = total
    if last:
        by_step = jnp.sum(jnp.concatenate(sums).T, axis=0, keepdims=True)
        sums_ref[0:1, :] = by_step
        sums_ref[1:2, :] = jnp.full(by_step.shape, jnp.sum(w_ref[...]), jnp.float32)
        sums_ref[2:, :] = jnp.zeros((SUBLANES - 2, by_step.shape[1]), jnp.float32)
    for copy in copies:
        copy.wait()


def depart(chunk, day, x, w, recv, own, before, out):
    tiles, rows = x.shape[0], x.shape[1] // CHUNKS
    steps, last = tiles * SUBLANES, chunk == CHUNKS - 1
    inputs, specs, aliases = [day, x, w, recv, own], [SMEM] + [VMEM] * 4, {}
    if chunk > 0:
        inputs, specs, aliases = inputs + [before, out], specs + [VMEM, HBM], {6: 0}
    return local_call(
        functools.partial(depart_kernel, chunk, last),
        f"depart_{chunk}",
        (pltpu.HBM((tiles, rows * CHUNKS, LANES), jnp.float32), vmem(SUBLANES if last else steps, steps if last else LANES)),
        *inputs,
        in_specs=specs,
        out_specs=(HBM, VMEM),
        scratch_shapes=[
            pltpu.VMEM((rows // 2 * tiles, LANES), jnp.float32),
            pltpu.VMEM((tiles, rows, LANES), jnp.float32),
            pltpu.SemaphoreType.DMA((PIECES,)),
        ],
        input_output_aliases=aliases,
        vmem=4 << 20,
    )


def exchange(x, pair, name):
    years, spaces = lax.axis_size("year"), lax.axis_size("space")
    partners = [(y * spaces + s, (y ^ pair[s % 2]) * spaces + s) for y in range(years) for s in range(spaces)]
    with jax.named_scope(name):
        return lax.ppermute(pltpu.with_memory_space_constraint(x, pltpu.VMEM), AXES, partners)


def day_tables(chunk, send, keep):
    pairs = stage_bits(chunk, lax.axis_size("year"))
    for stage, pair in enumerate(pairs):
        got = exchange(send if stage < HALVINGS else keep, pair, f"send_{chunk}_{stage}")
        yield
        name = f"merge_{chunk}_{stage}"
        if stage < HALVINGS - 1:
            half = vmem(*got.shape[1:])
            send, keep = local_call(merge_kernel, name, (half, half), got, keep, out_specs=(VMEM, VMEM))
        elif stage < len(pairs) - 1:
            keep = local_call(merge_kernel, name, vmem(*got.shape), got, keep, out_specs=VMEM)
    table = local_call(table_kernel, name, vmem(REST, 2 * SLOTS, *got.shape[-2:]), got, keep, out_specs=VMEM)
    for stage in reversed(range(HALVINGS)):
        number = len(pairs) + HALVINGS - 1 - stage
        got = exchange(table, pairs[stage], f"send_{chunk}_{number}")
        yield
        if stage > 0:
            table = local_call(join_kernel, f"merge_{chunk}_{number}", vmem(2, *got.shape), got, table, out_specs=VMEM)
    yield got, table


def on_device(thermal_reading, yearday_position, usable_observation_tally, location_surface_factor):
    steps, cells = thermal_reading.shape
    tiles, columns = steps // SUBLANES, cells // LANES
    x = thermal_reading.reshape(tiles, SUBLANES, columns, LANES).transpose(0, 2, 1, 3)
    x = x.reshape(tiles, columns * SUBLANES, LANES)
    w = location_surface_factor.reshape(columns, LANES)
    chunks = []
    for c in range(CHUNKS):
        send, keep, *copied = stats(c, yearday_position, usable_observation_tally, x)
        if copied:
            x = copied[0]
        chunks.append(day_tables(c, send, keep))
    results = [None] * CHUNKS
    while not all(results):
        for c in range(CHUNKS):
            results[c] = next(chunks[c])
    out = sums = None
    for c in range(CHUNKS):
        out, sums = depart(c, yearday_position, x, w, *results[c], sums, out)
    if lax.axis_size("space") == 2:
        sums += lax.ppermute(sums, "space", [(0, 1), (1, 0)])
    else:
        sums = lax.psum(sums, "space")
    out = out.reshape(tiles, columns, SUBLANES, LANES).transpose(0, 2, 1, 3).reshape(steps, cells)
    return out, sums[0] / sums[1]


def solution(mesh):
    return jax.shard_map(
        on_device,
        mesh=mesh,
        in_specs=(P("year", "space"), P("year"), P("year"), P("space")),
        out_specs=(P("year", "space"), P("year")),
        check_vma=False,
    )
```

```python
import functools
import math

import jax
import jax.numpy as jnp
from jax import lax
from jax.experimental import pallas as pl
from jax.experimental.pallas import tpu as pltpu
from jax.sharding import PartitionSpec as P

DAYS = 30
SUBLANES, LANES = 8, 128
GROUPS = 2
SLOTS = -(-DAYS // GROUPS)
CHUNKS = 2
HALVINGS = 2
REST = 2 * GROUPS >> HALVINGS
HOURS, HIGH, LOW, TILES = SLOTS, SLOTS + 1, 2 * SLOTS + 1, 3 * SLOTS + 1
ORDERS = (((1, 0), (0, 1), (2, 3), (3, 2)), ((0, 2), (1, 3), (3, 1), (2, 0)))
AXES = ("year", "space")
PIECES = 4

VMEM = pl.BlockSpec(memory_space=pltpu.VMEM)
SMEM = pl.BlockSpec(memory_space=pltpu.SMEM)
HBM = pl.BlockSpec(memory_space=pltpu.HBM)


def local_call(kernel, name, out_shape, *inputs, **options):
    specs = options.pop("in_specs", [VMEM] * len(inputs))
    spaces = {id(VMEM): pltpu.VMEM, id(HBM): pltpu.HBM}
    inputs = [pltpu.with_memory_space_constraint(a, spaces[id(s)]) if id(s) in spaces else a for a, s in zip(inputs, specs)]
    limit = pltpu.CompilerParams(vmem_limit_bytes=options.pop("vmem", 1 << 20))
    return pl.pallas_call(kernel, in_specs=specs, out_shape=out_shape, name=name, compiler_params=limit, **options)(*inputs)


def vmem(*shape):
    return pltpu.VMEM(shape, jnp.float32)


def stage_bits(chunk, years):
    assert HALVINGS > 1 and 2 * GROUPS >= 1 << HALVINGS and SLOTS <= 2 * SUBLANES
    count = years.bit_length() - 1
    assert years == 1 << count and count > HALVINGS
    return [tuple(1 << b for b in pair) for pair in ORDERS[chunk]] + [(1 << b, 1 << b) for b in range(4, count)]


def own_bits(chunk):
    year, core = lax.axis_index("year"), lax.rem(lax.axis_index("space"), 2)
    pairs = stage_bits(chunk, lax.axis_size("year"))[:HALVINGS]
    return [jnp.where(core == 0, year // a % 2, year // b % 2) for a, b in pairs]


def day_flip(bits):
    return sum((1 - bit) * (GROUPS >> i) for i, bit in enumerate(bits) if i > 0)


def place(day, flip):
    group = sum((day >= g * SLOTS).astype(jnp.int32) for g in range(1, GROUPS))
    return lax.bitwise_xor(group, flip), day - group * SLOTS


def by_group(*refs):
    return [ref.reshape(math.prod(ref.shape[:-3]), *ref.shape[-3:]) if len(ref.shape) > 3 else ref for ref in refs]


def stats_kernel(chunk, *refs):
    if chunk == 0:
        day_in, tally_in, x_in, send_ref, keep_ref, x_ref, day_ref, tally_ref, hours, arrived, listed = refs
        tiles, rows = x_in.shape[0], x_in.shape[1] // CHUNKS
        piece = tiles // PIECES
        lists = [pltpu.make_async_copy(day_in, day_ref, listed.at[0]), pltpu.make_async_copy(tally_in, tally_ref, listed.at[1])]
        copies = []
        for c in range(CHUNKS):
            for p in range(PIECES):
                at = pl.ds(p * piece, piece), pl.ds(c * rows, rows)
                copies.append(pltpu.make_async_copy(x_in.at[at], x_ref.at[at], arrived.at[c, p]))
        for copy in lists + copies:
            copy.start()
    else:
        day_ref, tally_ref, x_ref, send_ref, keep_ref, hours = refs
        tiles, rows = x_ref.shape[0], x_ref.shape[1] // CHUNKS
        piece, lists, copies = tiles // PIECES, [], []
    bits = own_bits(chunk)
    flip = day_flip(bits)
    half = rows // 2
    height = half // SUBLANES
    outs = by_group(send_ref, keep_ref)
    starts = [chunk * rows + (1 - bits[0]) * half, chunk * rows + bits[0] * half]
    for out in outs:
        for slot in range(GROUPS):
            block = out.at[slot]
            block[:HIGH] = jnp.zeros((HIGH, height, LANES), jnp.float32)
            block[HIGH:LOW] = jnp.full((SLOTS, height, LANES), -jnp.inf, jnp.float32)
            block[LOW:] = jnp.full((SLOTS, height, LANES), jnp.inf, jnp.float32)
    for d in range(GROUPS * SLOTS):
        hours[d] = 0
    for copy in lists:
        copy.wait()

    def tile(t, carry):
        for k in range(SUBLANES):
            step = t * SUBLANES + k
            day, tally = day_ref[step], tally_ref[step]
            slot, index = place(day, flip)
            hours[day] += tally
            tally = tally.astype(jnp.float32)
            blocks = [out.at[slot] for out in outs]
            x = [x_ref[t, pl.ds(start + k, height, stride=SUBLANES), :] for start in starts]
            old = [[b[index], b[HIGH + index], b[LOW + index]] for b in blocks]
            new = [[o[0] + tally * v, jnp.maximum(o[1], v), jnp.minimum(o[2], v)] for o, v in zip(old, x)]
            for b, n in zip(blocks, new):
                b[index], b[HIGH + index], b[LOW + index] = n
        return carry

    for p in range(PIECES):
        if copies:
            copies[p].wait()
        lax.fori_loop(p * piece, (p + 1) * piece, tile, 0)
    left = lax.broadcasted_iota(jnp.int32, (1, LANES), 1) < LANES // 2
    for group in range(GROUPS):
        slot = lax.bitwise_xor(group, flip)
        for k in range(SUBLANES):
            pair = [hours[group * SLOTS + min(i, SLOTS - 1)].astype(jnp.float32) for i in (k, k + SUBLANES)]
            for out in outs:
                out[slot, HOURS, k : k + 1, :] = jnp.where(left, *pair)
    for copy in copies[PIECES:]:
        copy.wait()


def stats(chunk, day, tally, x):
    tiles, rows = x.shape[0], x.shape[1] // CHUNKS
    half = vmem(*(2,) * (HALVINGS - 1), REST, TILES, rows // 2 // SUBLANES, LANES)
    shapes, scratch = (half, half), [pltpu.SMEM((GROUPS * SLOTS,), jnp.int32)]
    if chunk == 0:
        shapes += (vmem(*x.shape),)
        lists = [pltpu.SMEM(day.shape, jnp.int32)] * 2
        scratch = lists + scratch + [pltpu.SemaphoreType.DMA((CHUNKS, PIECES)), pltpu.SemaphoreType.DMA((2,))]
    return local_call(
        functools.partial(stats_kernel, chunk),
        f"stats_{chunk}",
        shapes,
        day, tally, x,
        in_specs=[HBM] * 3 if chunk == 0 else [SMEM, SMEM, VMEM],
        out_specs=(VMEM,) * len(shapes),
        scratch_shapes=scratch,
    )


def merge_kernel(got_ref, own_ref, *out_refs):
    got, own, *outs = by_group(got_ref, own_ref, *out_refs)
    each = got.shape[0] // len(outs)
    for i in range(got.shape[0]):
        for a, b, join in ((0, HIGH, jnp.add), (HIGH, LOW, jnp.maximum), (LOW, TILES, jnp.minimum)):
            outs[i // each][i % each, a:b] = join(got[i, a:b], own[i, a:b])


def table_kernel(got_ref, own_ref, table_ref):
    for g in range(REST):
        got, own, table = got_ref.at[g], own_ref.at[g], table_ref.at[g]
        hours = got[HOURS] + own[HOURS]
        left = lax.broadcasted_iota(jnp.int32, hours.shape, 1) < LANES // 2
        other = pltpu.roll(hours, LANES // 2, axis=1)
        hours = jnp.concatenate([jnp.where(left, hours, other), jnp.where(left, other, hours)])
        for i in range(SLOTS):
            total = got[i] + own[i]
            table[i] = total / jnp.broadcast_to(hours[i : i + 1], total.shape)
            high = jnp.maximum(got[HIGH + i], own[HIGH + i])
            low = jnp.minimum(got[LOW + i], own[LOW + i])
            table[SLOTS + i] = 4.0 / (high - low + 1.0)


def join_kernel(got_ref, own_ref, out_ref):
    out_ref[0] = got_ref[...]
    out_ref[1] = own_ref[...]


def depart_kernel(chunk, last, day_ref, x_ref, w_ref, recv_ref, own_ref, *refs):
    earlier, refs = refs[: 2 * chunk], refs[2 * chunk :]
    out_ref, sums_ref, *refs = refs
    copies = []
    if last:
        whole_ref, squares, left = refs
        rows = out_ref.shape[1]
        for c, ref in enumerate(earlier[1::2]):
            copies.append(pltpu.make_async_copy(ref, whole_ref.at[:, pl.ds(c * rows, rows)], left.at[c]))
            copies[-1].start()
    else:
        (squares,) = refs
    tiles, rows = out_ref.shape[0], out_ref.shape[1]
    bits = own_bits(chunk)
    flip = day_flip(bits)
    tables = by_group(recv_ref, own_ref)
    half_rows = rows // 2
    height = half_rows // SUBLANES
    starts = [(1 - bits[0]) * half_rows, bits[0] * half_rows]
    weights = [w_ref[pl.ds(pl.multiple_of((chunk * 2 + b) * height, height), height), :] for b in (1 - bits[0], bits[0])]

    def tile(t, carry):
        for k in range(SUBLANES):
            slot, index = place(day_ref[t * SUBLANES + k], flip)
            total = None
            for half, table_ref in enumerate(tables):
                at = starts[half] + k
                table = table_ref.at[slot]
                x = x_ref[t, pl.ds(chunk * rows + at, height, stride=SUBLANES), :]
                departure = (x - table[index]) * table[SLOTS + index]
                out_ref[t, pl.ds(at, height, stride=SUBLANES), :] = departure
                square = weights[half] * departure * departure
                total = square if total is None else total + square
            squares[pl.ds(pl.multiple_of((t * SUBLANES + k) * height, height), height), :] = total
        return carry

    lax.fori_loop(0, tiles, tile, 0)
    sums = []
    for t in range(tiles):
        start = t * SUBLANES * height
        total = squares[pl.ds(start, SUBLANES, stride=height), :]
        for j in range(1, height):
            total += squares[pl.ds(start + j, SUBLANES, stride=height), :]
        at = pl.ds(t * SUBLANES, SUBLANES)
        for before_ref in earlier[::2]:
            total += before_ref[at, :]
        if last:
            sums.append(total)
        else:
            sums_ref[at, :] = total
    if last:
        by_step = jnp.sum(jnp.concatenate(sums).T, axis=0, keepdims=True)
        sums_ref[0:1, :] = by_step
        sums_ref[1:2, :] = jnp.full(by_step.shape, jnp.sum(w_ref[...]), jnp.float32)
        sums_ref[2:, :] = jnp.zeros((SUBLANES - 2, by_step.shape[1]), jnp.float32)
    for copy in copies:
        copy.wait()


def depart(chunk, day, x, w, recv, own, earlier):
    tiles, rows = x.shape[0], x.shape[1] // CHUNKS
    steps, last = tiles * SUBLANES, chunk == CHUNKS - 1
    shapes = (vmem(tiles, rows, LANES), vmem(SUBLANES if last else steps, steps if last else LANES))
    specs, scratch = (VMEM, VMEM), [pltpu.VMEM((rows // 2 * tiles, LANES), jnp.float32)]
    if last:
        shapes, specs = shapes + (pltpu.HBM(x.shape, jnp.float32),), specs + (HBM,)
        scratch.append(pltpu.SemaphoreType.DMA((chunk,)))
    inputs = [day, x, w, recv, own, *earlier]
    return local_call(
        functools.partial(depart_kernel, chunk, last),
        f"depart_{chunk}",
        shapes,
        *inputs,
        in_specs=[SMEM] + [VMEM] * (len(inputs) - 1),
        out_specs=specs,
        scratch_shapes=scratch,
    )


def emit_kernel(part_ref, before_ref, out_ref, left):
    tiles, rows = part_ref.shape[0], part_ref.shape[1]
    piece, copies = tiles // PIECES, []
    for p in range(PIECES):
        at = pl.ds(p * piece, piece)
        here = out_ref.at[at, pl.ds(out_ref.shape[1] - rows, rows)]
        copies.append(pltpu.make_async_copy(part_ref.at[at], here, left.at[p]))
        copies[-1].start()
    for copy in copies:
        copy.wait()


def emit(part, out):
    return local_call(
        emit_kernel,
        "emit",
        pltpu.HBM(out.shape, jnp.float32),
        part, out,
        in_specs=[VMEM, HBM],
        out_specs=HBM,
        scratch_shapes=[pltpu.SemaphoreType.DMA((PIECES,))],
        input_output_aliases={1: 0},
    )


def exchange(x, pair, name):
    years, spaces = lax.axis_size("year"), lax.axis_size("space")
    partners = [(y * spaces + s, (y ^ pair[s % 2]) * spaces + s) for y in range(years) for s in range(spaces)]
    with jax.named_scope(name):
        return lax.ppermute(pltpu.with_memory_space_constraint(x, pltpu.VMEM), AXES, partners)


def day_tables(chunk, send, keep):
    pairs = stage_bits(chunk, lax.axis_size("year"))
    for stage, pair in enumerate(pairs):
        got = exchange(send if stage < HALVINGS else keep, pair, f"send_{chunk}_{stage}")
        yield
        name = f"merge_{chunk}_{stage}"
        if stage < HALVINGS - 1:
            half = vmem(*got.shape[1:])
            send, keep = local_call(merge_kernel, name, (half, half), got, keep, out_specs=(VMEM, VMEM))
        elif stage < len(pairs) - 1:
            keep = local_call(merge_kernel, name, vmem(*got.shape), got, keep, out_specs=VMEM)
    table = local_call(table_kernel, name, vmem(REST, 2 * SLOTS, *got.shape[-2:]), got, keep, out_specs=VMEM)
    for stage in reversed(range(HALVINGS)):
        number = len(pairs) + HALVINGS - 1 - stage
        got = exchange(table, pairs[stage], f"send_{chunk}_{number}")
        yield
        if stage > 0:
            table = local_call(join_kernel, f"merge_{chunk}_{number}", vmem(2, *got.shape), got, table, out_specs=VMEM)
    yield got, table


def on_device(thermal_reading, yearday_position, usable_observation_tally, location_surface_factor):
    steps, cells = thermal_reading.shape
    tiles, columns = steps // SUBLANES, cells // LANES
    x = thermal_reading.reshape(tiles, SUBLANES, columns, LANES).transpose(0, 2, 1, 3)
    x = x.reshape(tiles, columns * SUBLANES, LANES)
    w = location_surface_factor.reshape(columns, LANES)
    chunks = []
    for c in range(CHUNKS):
        send, keep, *copied = stats(c, yearday_position, usable_observation_tally, x)
        if copied:
            x = copied[0]
        chunks.append(day_tables(c, send, keep))
    results = [None] * CHUNKS
    while not all(results):
        for c in range(CHUNKS):
            results[c] = next(chunks[c])
    earlier = []
    for c in range(CHUNKS):
        part, sums, *whole = depart(c, yearday_position, x, w, *results[c], earlier)
        earlier += [sums, part]
    out = emit(part, *whole)
    if lax.axis_size("space") == 2:
        sums += lax.ppermute(sums, "space", [(0, 1), (1, 0)])
    else:
        sums = lax.psum(sums, "space")
    out = out.reshape(tiles, columns, SUBLANES, LANES).transpose(0, 2, 1, 3).reshape(steps, cells)
    return out, sums[0] / sums[1]


def solution(mesh):
    return jax.shard_map(
        on_device,
        mesh=mesh,
        in_specs=(P("year", "space"), P("year"), P("year"), P("space")),
        out_specs=(P("year", "space"), P("year")),
        check_vma=False,
    )
```

```python
import functools
import math

import jax
import jax.numpy as jnp
from jax import lax
from jax.experimental import pallas as pl
from jax.experimental.pallas import tpu as pltpu
from jax.sharding import PartitionSpec as P

DAYS = 30
SUBLANES, LANES = 8, 128
CHUNKS = 3
SLOTS = -(-DAYS // CHUNKS)
BLOCKS = 4
HALVINGS = 2
HOURS, HIGH, LOW, TILES = SLOTS, SLOTS + 1, 2 * SLOTS + 1, 3 * SLOTS + 1
ORDERS = (((2, 1), (0, 3), (1, 0), (3, 2)), ((0, 1), (1, 3), (3, 2), (2, 0)), ((0, 1), (1, 3), (3, 2), (2, 0)))
AXES = ("year", "space")
PIECES = 4

VMEM = pl.BlockSpec(memory_space=pltpu.VMEM)
SMEM = pl.BlockSpec(memory_space=pltpu.SMEM)
HBM = pl.BlockSpec(memory_space=pltpu.HBM)


def local_call(kernel, name, out_shape, *inputs, **options):
    specs = options.pop("in_specs", [VMEM] * len(inputs))
    spaces = {id(VMEM): pltpu.VMEM, id(HBM): pltpu.HBM}
    inputs = [pltpu.with_memory_space_constraint(a, spaces[id(s)]) if id(s) in spaces else a for a, s in zip(inputs, specs)]
    limit = pltpu.CompilerParams(vmem_limit_bytes=options.pop("vmem", 1 << 20))
    return pl.pallas_call(kernel, in_specs=specs, out_shape=out_shape, name=name, compiler_params=limit, **options)(*inputs)


def vmem(*shape):
    return pltpu.VMEM(shape, jnp.float32)


def stage_bits(chunk, years):
    assert BLOCKS == 1 << HALVINGS and SLOTS <= 2 * SUBLANES
    count = years.bit_length() - 1
    assert years == 1 << count and count > HALVINGS
    return [tuple(1 << b for b in pair) for pair in ORDERS[chunk]] + [(1 << b, 1 << b) for b in range(4, count)]


def block_of(chunk):
    year, core = lax.axis_index("year"), lax.rem(lax.axis_index("space"), 2)
    pairs = stage_bits(chunk, lax.axis_size("year"))[:HALVINGS]
    high, low = [jnp.where(core == 0, year // a % 2, year // b % 2) for a, b in pairs]
    return [[2 * p + r for r in (1 - low, low)] for p in (1 - high, high)]


def place(day):
    chunk = sum((day >= c * SLOTS).astype(jnp.int32) for c in range(1, CHUNKS))
    return chunk, day - chunk * SLOTS


def stats_kernel(day_in, tally_in, x_in, *refs):
    outs, (x_ref, day_ref, tally_ref, hours, totals, arrived, listed) = refs[: 2 * CHUNKS], refs[2 * CHUNKS :]
    tiles, rows = x_in.shape[0], x_in.shape[1] // BLOCKS
    piece = tiles // PIECES
    height = rows // SUBLANES
    lists = [pltpu.make_async_copy(day_in, day_ref, listed.at[0]), pltpu.make_async_copy(tally_in, tally_ref, listed.at[1])]
    copies = []
    for p in range(PIECES):
        at = pl.ds(p * piece, piece)
        copies.append(pltpu.make_async_copy(x_in.at[at], x_ref.at[at], arrived.at[p]))
    for copy in lists + copies:
        copy.start()
    for i in range(CHUNKS * BLOCKS):
        at = i * TILES
        totals[at : at + HIGH] = jnp.zeros((HIGH, height, LANES), jnp.float32)
        totals[at + HIGH : at + LOW] = jnp.full((SLOTS, height, LANES), -jnp.inf, jnp.float32)
        totals[at + LOW : at + TILES] = jnp.full((SLOTS, height, LANES), jnp.inf, jnp.float32)
    for d in range(CHUNKS * SLOTS):
        hours[d] = 0
    for copy in lists:
        copy.wait()

    def tile(t, carry):
        for k in range(SUBLANES):
            step = t * SUBLANES + k
            day, tally = day_ref[step], tally_ref[step]
            chunk, index = place(day)
            base = chunk * (BLOCKS * TILES) + index
            hours[day] += tally
            tally = tally.astype(jnp.float32)
            x = [x_ref[t, pl.ds(b * rows + k, height, stride=SUBLANES), :] for b in range(BLOCKS)]
            at = [[base + b * TILES + kind for kind in (0, HIGH, LOW)] for b in range(BLOCKS)]
            old = [[totals[i] for i in a] for a in at]
            new = [[o[0] + tally * v, jnp.maximum(o[1], v), jnp.minimum(o[2], v)] for o, v in zip(old, x)]
            for a, n in zip(at, new):
                for i, v in zip(a, n):
                    totals[i] = v
        return carry

    for p in range(PIECES):
        copies[p].wait()
        lax.fori_loop(p * piece, (p + 1) * piece, tile, 0)
    left = lax.broadcasted_iota(jnp.int32, (1, LANES), 1) < LANES // 2
    for c in range(CHUNKS):
        blocks = block_of(c)
        pairs = []
        for k in range(SUBLANES):
            pairs.append([hours[c * SLOTS + min(i, SLOTS - 1)].astype(jnp.float32) for i in (k, k + SUBLANES)])
        for half in range(2):
            for slot in range(2):
                out, start = outs[2 * c + half].at[slot], (c * BLOCKS + blocks[half][slot]) * TILES
                out[...] = totals[pl.ds(start, TILES)]
                for k, pair in enumerate(pairs):
                    out[HOURS, k : k + 1, :] = jnp.where(left, *pair)


def stats(day, tally, x):
    tiles, rows = x.shape[0], x.shape[1] // BLOCKS
    height = rows // SUBLANES
    shapes = (vmem(2, TILES, height, LANES),) * (2 * CHUNKS) + (vmem(*x.shape),)
    return local_call(
        stats_kernel,
        "stats",
        shapes,
        day, tally, x,
        in_specs=[HBM] * 3,
        out_specs=(VMEM,) * len(shapes),
        scratch_shapes=[
            pltpu.SMEM(day.shape, jnp.int32),
            pltpu.SMEM(day.shape, jnp.int32),
            pltpu.SMEM((CHUNKS * SLOTS,), jnp.int32),
            vmem(CHUNKS * BLOCKS * TILES, height, LANES),
            pltpu.SemaphoreType.DMA((PIECES,)),
            pltpu.SemaphoreType.DMA((2,)),
        ],
        vmem=8 << 20,
    )


def merge_kernel(got_ref, own_ref, *outs):
    for a, b, join in ((0, HIGH, jnp.add), (HIGH, LOW, jnp.maximum), (LOW, TILES, jnp.minimum)):
        for i, out in enumerate(outs):
            got, own = (got_ref.at[i], own_ref.at[i]) if len(outs) > 1 else (got_ref, own_ref)
            out[a:b] = join(got[a:b], own[a:b])


def table_kernel(got, own, table):
    hours = got[HOURS] + own[HOURS]
    left = lax.broadcasted_iota(jnp.int32, hours.shape, 1) < LANES // 2
    other = pltpu.roll(hours, LANES // 2, axis=1)
    hours = jnp.concatenate([jnp.where(left, hours, other), jnp.where(left, other, hours)])
    for i in range(SLOTS):
        total = got[i] + own[i]
        table[i] = total / jnp.broadcast_to(hours[i : i + 1], total.shape)
        high = jnp.maximum(got[HIGH + i], own[HIGH + i])
        low = jnp.minimum(got[LOW + i], own[LOW + i])
        table[SLOTS + i] = 4.0 / (high - low + 1.0)


def join_kernel(got_ref, own_ref, out_ref):
    out_ref[0] = got_ref[...]
    out_ref[1] = own_ref[...]


def depart_kernel(day_ref, x_ref, w_ref, *refs):
    tables, (last_ref, sums_ref, whole_ref, table, ready, squares, left) = refs[: 2 * CHUNKS], refs[2 * CHUNKS :]
    tiles, rows = x_ref.shape[0], x_ref.shape[1] // BLOCKS
    piece = tiles // PIECES
    height = rows // SUBLANES
    for c in range(CHUNKS):
        blocks = block_of(c)
        for half in range(2):
            for slot in range(2):
                start = (c * BLOCKS + blocks[half][slot]) * 2 * SLOTS
                table[pl.ds(start, 2 * SLOTS)] = tables[2 * c + half][slot]
    weights = [w_ref[b * height : (b + 1) * height, :] for b in range(BLOCKS)]

    def tile(first, out_ref, t, carry):
        for k in range(SUBLANES):
            chunk, index = place(day_ref[t * SUBLANES + k])
            base = chunk * (BLOCKS * 2 * SLOTS) + index
            total = None
            for b in range(BLOCKS):
                at = pl.ds(b * rows + k, height, stride=SUBLANES)
                mean, scale = table[base + b * 2 * SLOTS], table[base + (b * 2 + 1) * SLOTS]
                departure = (x_ref[t, at, :] - mean) * scale
                out_ref[t - first, at, :] = departure
                square = weights[b] * departure * departure
                total = square if total is None else total + square
            squares[pl.ds(pl.multiple_of((t * SUBLANES + k) * height, height), height), :] = total
        return carry

    copies = []
    for p in range(PIECES):
        first, final = p * piece, p == PIECES - 1
        out = last_ref if final else ready
        lax.fori_loop(first, first + piece, functools.partial(tile, first if final else 0, out), 0)
        if not final:
            at = pl.ds(first, piece)
            copies.append(pltpu.make_async_copy(ready.at[at], whole_ref.at[at], left.at[p]))
            copies[-1].start()
    sums = []
    for t in range(tiles):
        start = t * SUBLANES * height
        total = squares[pl.ds(start, SUBLANES, stride=height), :]
        for j in range(1, height):
            total += squares[pl.ds(start + j, SUBLANES, stride=height), :]
        sums.append(total)
    by_step = jnp.sum(jnp.concatenate(sums).T, axis=0, keepdims=True)
    sums_ref[0:1, :] = by_step
    sums_ref[1:2, :] = jnp.full(by_step.shape, jnp.sum(w_ref[...]), jnp.float32)
    sums_ref[2:, :] = jnp.zeros((SUBLANES - 2, by_step.shape[1]), jnp.float32)
    for copy in copies:
        copy.wait()


def depart(day, x, w, tables):
    tiles, rows = x.shape[0], x.shape[1] // BLOCKS
    height, piece, steps = rows // SUBLANES, tiles // PIECES, tiles * SUBLANES
    inputs = [day, x, w, *tables]
    return local_call(
        depart_kernel,
        "depart",
        (vmem(piece, *x.shape[1:]), vmem(SUBLANES, steps), pltpu.HBM(x.shape, jnp.float32)),
        *inputs,
        in_specs=[SMEM] + [VMEM] * (len(inputs) - 1),
        out_specs=(VMEM, VMEM, HBM),
        scratch_shapes=[
            vmem(CHUNKS * BLOCKS * 2 * SLOTS, height, LANES),
            vmem(tiles - piece, *x.shape[1:]),
            vmem(steps * height, LANES),
            pltpu.SemaphoreType.DMA((PIECES - 1,)),
        ],
        vmem=8 << 20,
    )


def emit_kernel(part_ref, before_ref, out_ref, left):
    piece, tiles = part_ref.shape[0], out_ref.shape[0]
    copies = []
    for i in range(piece):
        copies.append(pltpu.make_async_copy(part_ref.at[i], out_ref.at[tiles - piece + i], left.at[i]))
        copies[-1].start()
    for copy in copies:
        copy.wait()


def emit(part, out):
    return local_call(
        emit_kernel,
        "emit",
        pltpu.HBM(out.shape, jnp.float32),
        part, out,
        in_specs=[VMEM, HBM],
        out_specs=HBM,
        scratch_shapes=[pltpu.SemaphoreType.DMA((part.shape[0],))],
        input_output_aliases={1: 0},
    )


def exchange(x, pair, name):
    years, spaces = lax.axis_size("year"), lax.axis_size("space")
    partners = [(y * spaces + s, (y ^ pair[s % 2]) * spaces + s) for y in range(years) for s in range(spaces)]
    with jax.named_scope(name):
        return lax.ppermute(pltpu.with_memory_space_constraint(x, pltpu.VMEM), AXES, partners)


def day_tables(chunk, send, keep):
    pairs = stage_bits(chunk, lax.axis_size("year"))
    for stage, pair in enumerate(pairs):
        got = exchange(send if stage < HALVINGS else keep, pair, f"send_{chunk}_{stage}")
        yield
        name = f"merge_{chunk}_{stage}"
        if stage < HALVINGS - 1:
            half = vmem(*got.shape[1:])
            send, keep = local_call(merge_kernel, name, (half, half), got, keep, out_specs=(VMEM, VMEM))
        elif stage < len(pairs) - 1:
            keep = local_call(merge_kernel, name, vmem(*got.shape), got, keep, out_specs=VMEM)
    table = local_call(table_kernel, name, vmem(2 * SLOTS, *got.shape[1:]), got, keep, out_specs=VMEM)
    for stage in reversed(range(HALVINGS)):
        number = len(pairs) + HALVINGS - 1 - stage
        got = exchange(table, pairs[stage], f"send_{chunk}_{number}")
        yield
        if stage > 0:
            table = local_call(join_kernel, f"merge_{chunk}_{number}", vmem(2, *got.shape), got, table, out_specs=VMEM)
    yield got, table


def on_device(thermal_reading, yearday_position, usable_observation_tally, location_surface_factor):
    steps, cells = thermal_reading.shape
    tiles, columns = steps // SUBLANES, cells // LANES
    x = thermal_reading.reshape(tiles, SUBLANES, columns, LANES).transpose(0, 2, 1, 3)
    x = x.reshape(tiles, columns * SUBLANES, LANES)
    w = location_surface_factor.reshape(columns, LANES)
    *halves, x = stats(yearday_position, usable_observation_tally, x)
    chunks = [day_tables(c, *halves[2 * c : 2 * c + 2]) for c in range(CHUNKS)]
    results = [None] * CHUNKS
    while not all(results):
        for c in range(CHUNKS):
            results[c] = next(chunks[c])
    part, sums, out = depart(yearday_position, x, w, [table for pair in results for table in pair])
    out = emit(part, out)
    if lax.axis_size("space") == 2:
        sums += lax.ppermute(sums, "space", [(0, 1), (1, 0)])
    else:
        sums = lax.psum(sums, "space")
    out = out.reshape(tiles, columns, SUBLANES, LANES).transpose(0, 2, 1, 3).reshape(steps, cells)
    return out, sums[0] / sums[1]


def solution(mesh):
    return jax.shard_map(
        on_device,
        mesh=mesh,
        in_specs=(P("year", "space"), P("year"), P("year"), P("space")),
        out_specs=(P("year", "space"), P("year")),
        check_vma=False,
    )
```

```python
import functools
import math

import jax
import jax.numpy as jnp
from jax import lax
from jax.experimental import pallas as pl
from jax.experimental.pallas import tpu as pltpu
from jax.sharding import PartitionSpec as P

DAYS = 30
SUBLANES, LANES = 8, 128
CHUNKS = 3
SLOTS = -(-DAYS // CHUNKS)
BLOCKS = 4
HALVINGS = 2
HOURS, HIGH, LOW, TILES = SLOTS, SLOTS + 1, 2 * SLOTS + 1, 3 * SLOTS + 1
KINDS = (0, HIGH, jnp.add), (HIGH, LOW, jnp.maximum), (LOW, TILES, jnp.minimum)
ORDERS = (((2, 1), (0, 3), (1, 0), (3, 2)), ((0, 1), (1, 3), (3, 2), (2, 0)), ((0, 1), (1, 3), (3, 2), (2, 0)))
AXES = ("year", "space")
PIECES = 4
LATE = 2
TOGETHER = 4

VMEM = pl.BlockSpec(memory_space=pltpu.VMEM)
SMEM = pl.BlockSpec(memory_space=pltpu.SMEM)
HBM = pl.BlockSpec(memory_space=pltpu.HBM)


def local_call(kernel, name, out_shape, *inputs, **options):
    specs = options.pop("in_specs", [VMEM] * len(inputs))
    spaces = {id(VMEM): pltpu.VMEM, id(HBM): pltpu.HBM}
    inputs = [pltpu.with_memory_space_constraint(a, spaces[id(s)]) if id(s) in spaces else a for a, s in zip(inputs, specs)]
    limit = pltpu.CompilerParams(vmem_limit_bytes=options.pop("vmem", 1 << 20))
    return pl.pallas_call(kernel, in_specs=specs, out_shape=out_shape, name=name, compiler_params=limit, **options)(*inputs)


def vmem(*shape):
    return pltpu.VMEM(shape, jnp.float32)


def stage_bits(chunk, years):
    assert BLOCKS == 1 << HALVINGS and SLOTS <= 2 * SUBLANES
    count = years.bit_length() - 1
    assert years == 1 << count and count > HALVINGS
    return [tuple(1 << b for b in pair) for pair in ORDERS[chunk]] + [(1 << b, 1 << b) for b in range(4, count)]


def block_of(chunk):
    year, core = lax.axis_index("year"), lax.rem(lax.axis_index("space"), 2)
    pairs = stage_bits(chunk, lax.axis_size("year"))[:HALVINGS]
    high, low = [jnp.where(core == 0, year // a % 2, year // b % 2) for a, b in pairs]
    return [[2 * p + r for r in (1 - low, low)] for p in (1 - high, high)]


def place(day):
    chunk = sum((day >= c * SLOTS).astype(jnp.int32) for c in range(1, CHUNKS))
    return chunk, day - chunk * SLOTS


def stats_kernel(day_in, tally_in, x_in, *refs):
    outs, (x_ref, day_ref, tally_ref, hours, even, odd, arrived, listed) = refs[: 2 * CHUNKS], refs[2 * CHUNKS :]
    tiles, rows = x_in.shape[0], x_in.shape[1] // BLOCKS
    piece = tiles // PIECES
    height = rows // SUBLANES
    lists = [pltpu.make_async_copy(day_in, day_ref, listed.at[0]), pltpu.make_async_copy(tally_in, tally_ref, listed.at[1])]
    copies = []
    for p in range(PIECES):
        at = pl.ds(p * piece, piece)
        copies.append(pltpu.make_async_copy(x_in.at[at], x_ref.at[at], arrived.at[p]))
    for copy in lists + copies:
        copy.start()
    for i in range(CHUNKS * BLOCKS):
        at = i * TILES
        for totals in (even, odd):
            totals[at : at + HIGH] = jnp.zeros((HIGH, height, LANES), jnp.float32)
            totals[at + HIGH : at + LOW] = jnp.full((SLOTS, height, LANES), -jnp.inf, jnp.float32)
            totals[at + LOW : at + TILES] = jnp.full((SLOTS, height, LANES), jnp.inf, jnp.float32)
    for d in range(CHUNKS * SLOTS):
        hours[d] = 0
    for copy in lists:
        copy.wait()

    def tile(t, carry):
        for k in range(SUBLANES):
            step, totals = t * SUBLANES + k, odd if k % 2 else even
            day, tally = day_ref[step], tally_ref[step]
            chunk, index = place(day)
            base = chunk * (BLOCKS * TILES) + index
            hours[day] += tally
            tally = tally.astype(jnp.float32)
            x = [x_ref[t, pl.ds(b * rows + k, height, stride=SUBLANES), :] for b in range(BLOCKS)]
            at = [[base + b * TILES + kind for kind in (0, HIGH, LOW)] for b in range(BLOCKS)]
            old = [[totals[i] for i in a] for a in at]
            new = [[o[0] + tally * v, jnp.maximum(o[1], v), jnp.minimum(o[2], v)] for o, v in zip(old, x)]
            for a, n in zip(at, new):
                for i, v in zip(a, n):
                    totals[i] = v
        return carry

    for p in range(PIECES):
        copies[p].wait()
        lax.fori_loop(p * piece, (p + 1) * piece, tile, 0)
    left = lax.broadcasted_iota(jnp.int32, (1, LANES), 1) < LANES // 2
    for c in range(CHUNKS):
        blocks = block_of(c)
        pairs = []
        for k in range(SUBLANES):
            pairs.append([hours[c * SLOTS + min(i, SLOTS - 1)].astype(jnp.float32) for i in (k, k + SUBLANES)])
        for half in range(2):
            for slot in range(2):
                out, start = outs[2 * c + half].at[slot], (c * BLOCKS + blocks[half][slot]) * TILES
                for a, b, join in KINDS:
                    at = pl.ds(start + a, b - a)
                    out[a:b] = join(even[at], odd[at])
                for k, pair in enumerate(pairs):
                    out[HOURS, k : k + 1, :] = jnp.where(left, *pair)


def stats(day, tally, x):
    tiles, rows = x.shape[0], x.shape[1] // BLOCKS
    height = rows // SUBLANES
    shapes = (vmem(2, TILES, height, LANES),) * (2 * CHUNKS) + (vmem(*x.shape),)
    return local_call(
        stats_kernel,
        "stats",
        shapes,
        day, tally, x,
        in_specs=[HBM] * 3,
        out_specs=(VMEM,) * len(shapes),
        scratch_shapes=[
            pltpu.SMEM(day.shape, jnp.int32),
            pltpu.SMEM(day.shape, jnp.int32),
            pltpu.SMEM((CHUNKS * SLOTS,), jnp.int32),
            vmem(CHUNKS * BLOCKS * TILES, height, LANES),
            vmem(CHUNKS * BLOCKS * TILES, height, LANES),
            pltpu.SemaphoreType.DMA((PIECES,)),
            pltpu.SemaphoreType.DMA((2,)),
        ],
        vmem=8 << 20,
    )


def merge_kernel(got_ref, own_ref, *outs):
    for a, b, join in KINDS:
        for i, out in enumerate(outs):
            got, own = (got_ref.at[i], own_ref.at[i]) if len(outs) > 1 else (got_ref, own_ref)
            out[a:b] = join(got[a:b], own[a:b])


def table_kernel(got, own, table):
    hours = got[HOURS] + own[HOURS]
    left = lax.broadcasted_iota(jnp.int32, hours.shape, 1) < LANES // 2
    other = pltpu.roll(hours, LANES // 2, axis=1)
    hours = jnp.concatenate([jnp.where(left, hours, other), jnp.where(left, other, hours)])
    for i in range(SLOTS):
        total = got[i] + own[i]
        table[i] = total / jnp.broadcast_to(hours[i : i + 1], total.shape)
        high = jnp.maximum(got[HIGH + i], own[HIGH + i])
        low = jnp.minimum(got[LOW + i], own[LOW + i])
        table[SLOTS + i] = 4.0 / (high - low + 1.0)


def join_kernel(got_ref, own_ref, out_ref):
    out_ref[0] = got_ref[...]
    out_ref[1] = own_ref[...]


def depart_kernel(day_in, x_ref, w_ref, *refs):
    tables, refs = refs[: 2 * CHUNKS], refs[2 * CHUNKS :]
    last_ref, sums_ref, whole_ref, table, ready, squares, left, day_ref, listed = refs
    days = pltpu.make_async_copy(day_in, day_ref, listed)
    days.start()
    tiles, rows = x_ref.shape[0], x_ref.shape[1] // BLOCKS
    piece = tiles // PIECES
    height = rows // SUBLANES
    for c in range(CHUNKS):
        blocks = block_of(c)
        for half in range(2):
            for slot in range(2):
                start = (c * BLOCKS + blocks[half][slot]) * 2 * SLOTS
                table[pl.ds(start, 2 * SLOTS)] = tables[2 * c + half][slot]
    days.wait()
    weights = [w_ref[b * height : (b + 1) * height, :] for b in range(BLOCKS)]

    def tile(first, out_ref, t, carry):
        for k in range(0, SUBLANES, TOGETHER):
            loaded = []
            for j in range(k, k + TOGETHER):
                chunk, index = place(day_ref[t * SUBLANES + j])
                base = chunk * (BLOCKS * 2 * SLOTS) + index
                for b in range(BLOCKS):
                    x = x_ref[t, pl.ds(b * rows + j, height, stride=SUBLANES), :]
                    loaded.append((x, table[base + b * 2 * SLOTS], table[base + (b * 2 + 1) * SLOTS]))
            for j in range(k, k + TOGETHER):
                total = None
                for b in range(BLOCKS):
                    x, mean, scale = loaded[(j - k) * BLOCKS + b]
                    departure = (x - mean) * scale
                    out_ref[t - first, pl.ds(b * rows + j, height, stride=SUBLANES), :] = departure
                    square = weights[b] * departure * departure
                    total = square if total is None else total + square
                squares[pl.ds(pl.multiple_of((t * SUBLANES + j) * height, height), height), :] = total
        return carry

    copies = []
    for p in range(PIECES):
        first, late = p * piece, p >= PIECES - LATE
        before = (PIECES - LATE) * piece if late else 0
        lax.fori_loop(first, first + piece, functools.partial(tile, before, last_ref if late else ready), 0)
        if not late:
            at = pl.ds(first, piece)
            copies.append(pltpu.make_async_copy(ready.at[at], whole_ref.at[at], left.at[p]))
            copies[-1].start()
    sums = []
    for t in range(tiles):
        start = t * SUBLANES * height
        total = squares[pl.ds(start, SUBLANES, stride=height), :]
        for j in range(1, height):
            total += squares[pl.ds(start + j, SUBLANES, stride=height), :]
        sums.append(total)
    by_step = jnp.sum(jnp.concatenate(sums).T, axis=0, keepdims=True)
    sums_ref[0:1, :] = by_step
    sums_ref[1:2, :] = jnp.full(by_step.shape, jnp.sum(w_ref[...]), jnp.float32)
    sums_ref[2:, :] = jnp.zeros((SUBLANES - 2, by_step.shape[1]), jnp.float32)
    for copy in copies:
        copy.wait()


def depart(day, x, w, tables):
    tiles, rows = x.shape[0], x.shape[1] // BLOCKS
    height, late, steps = rows // SUBLANES, tiles // PIECES * LATE, tiles * SUBLANES
    inputs = [day, x, w, *tables]
    return local_call(
        depart_kernel,
        "depart",
        (vmem(late, *x.shape[1:]), vmem(SUBLANES, steps), pltpu.HBM(x.shape, jnp.float32)),
        *inputs,
        in_specs=[VMEM] * len(inputs),
        out_specs=(VMEM, VMEM, HBM),
        scratch_shapes=[
            vmem(CHUNKS * BLOCKS * 2 * SLOTS, height, LANES),
            vmem(tiles - late, *x.shape[1:]),
            vmem(steps * height, LANES),
            pltpu.SemaphoreType.DMA((PIECES - LATE,)),
            pltpu.SMEM(day.shape, jnp.int32),
            pltpu.SemaphoreType.DMA,
        ],
        vmem=8 << 20,
    )


def emit_kernel(part_ref, before_ref, out_ref, left):
    piece, tiles = part_ref.shape[0], out_ref.shape[0]
    copies = []
    for i in range(piece):
        copies.append(pltpu.make_async_copy(part_ref.at[i], out_ref.at[tiles - piece + i], left.at[i]))
        copies[-1].start()
    for copy in copies:
        copy.wait()


def emit(part, out):
    return local_call(
        emit_kernel,
        "emit",
        pltpu.HBM(out.shape, jnp.float32),
        part, out,
        in_specs=[VMEM, HBM],
        out_specs=HBM,
        scratch_shapes=[pltpu.SemaphoreType.DMA((part.shape[0],))],
        input_output_aliases={1: 0},
    )


def exchange(x, pair, name):
    years, spaces = lax.axis_size("year"), lax.axis_size("space")
    partners = [(y * spaces + s, (y ^ pair[s % 2]) * spaces + s) for y in range(years) for s in range(spaces)]
    with jax.named_scope(name):
        return lax.ppermute(pltpu.with_memory_space_constraint(x, pltpu.VMEM), AXES, partners)


def day_tables(chunk, send, keep):
    pairs = stage_bits(chunk, lax.axis_size("year"))
    for stage, pair in enumerate(pairs):
        got = exchange(send if stage < HALVINGS else keep, pair, f"send_{chunk}_{stage}")
        yield
        name = f"merge_{chunk}_{stage}"
        if stage < HALVINGS - 1:
            half = vmem(*got.shape[1:])
            send, keep = local_call(merge_kernel, name, (half, half), got, keep, out_specs=(VMEM, VMEM))
        elif stage < len(pairs) - 1:
            keep = local_call(merge_kernel, name, vmem(*got.shape), got, keep, out_specs=VMEM)
    table = local_call(table_kernel, name, vmem(2 * SLOTS, *got.shape[1:]), got, keep, out_specs=VMEM)
    for stage in reversed(range(HALVINGS)):
        number = len(pairs) + HALVINGS - 1 - stage
        got = exchange(table, pairs[stage], f"send_{chunk}_{number}")
        yield
        if stage > 0:
            table = local_call(join_kernel, f"merge_{chunk}_{number}", vmem(2, *got.shape), got, table, out_specs=VMEM)
    yield got, table


def on_device(thermal_reading, yearday_position, usable_observation_tally, location_surface_factor):
    steps, cells = thermal_reading.shape
    tiles, columns = steps // SUBLANES, cells // LANES
    x = thermal_reading.reshape(tiles, SUBLANES, columns, LANES).transpose(0, 2, 1, 3)
    x = x.reshape(tiles, columns * SUBLANES, LANES)
    w = location_surface_factor.reshape(columns, LANES)
    *halves, x = stats(yearday_position, usable_observation_tally, x)
    chunks = [day_tables(c, *halves[2 * c : 2 * c + 2]) for c in range(CHUNKS)]
    results = [None] * CHUNKS
    while not all(results):
        for c in range(CHUNKS):
            results[c] = next(chunks[c])
    part, sums, out = depart(yearday_position, x, w, [table for pair in results for table in pair])
    out = emit(part, out)
    if lax.axis_size("space") == 2:
        sums += lax.ppermute(sums, "space", [(0, 1), (1, 0)])
    else:
        sums = lax.psum(sums, "space")
    out = out.reshape(tiles, columns, SUBLANES, LANES).transpose(0, 2, 1, 3).reshape(steps, cells)
    return out, sums[0] / sums[1]


def solution(mesh):
    return jax.shard_map(
        on_device,
        mesh=mesh,
        in_specs=(P("year", "space"), P("year"), P("year"), P("space")),
        out_specs=(P("year", "space"), P("year")),
        check_vma=False,
    )
```

```python
import functools
import math

import jax
import jax.numpy as jnp
from jax import lax
from jax.experimental import pallas as pl
from jax.experimental.pallas import tpu as pltpu
from jax.sharding import PartitionSpec as P

DAYS = 30
SUBLANES, LANES = 8, 128
CHUNKS = 3
SLOTS = -(-DAYS // CHUNKS)
BLOCKS = 4
HALVINGS = 2
HOURS, HIGH, LOW, TILES = SLOTS, SLOTS + 1, 2 * SLOTS + 1, 3 * SLOTS + 1
KINDS = (0, HIGH, jnp.add), (HIGH, LOW, jnp.maximum), (LOW, TILES, jnp.minimum)
ORDERS = (((2, 1), (0, 3), (1, 2), (3, 0)), ((0, 1), (1, 3), (3, 0), (2, 2)), ((2, 1), (0, 3), (3, 2), (1, 0)))
AXES = ("year", "space")
PIECES = 8
LATE = 4
TOGETHER = 4

VMEM = pl.BlockSpec(memory_space=pltpu.VMEM)
SMEM = pl.BlockSpec(memory_space=pltpu.SMEM)
HBM = pl.BlockSpec(memory_space=pltpu.HBM)


def local_call(kernel, name, out_shape, *inputs, **options):
    specs = options.pop("in_specs", [VMEM] * len(inputs))
    spaces = {id(VMEM): pltpu.VMEM, id(HBM): pltpu.HBM}
    inputs = [pltpu.with_memory_space_constraint(a, spaces[id(s)]) if id(s) in spaces else a for a, s in zip(inputs, specs)]
    limit = pltpu.CompilerParams(vmem_limit_bytes=options.pop("vmem", 1 << 20))
    return pl.pallas_call(kernel, in_specs=specs, out_shape=out_shape, name=name, compiler_params=limit, **options)(*inputs)


def vmem(*shape):
    return pltpu.VMEM(shape, jnp.float32)


def stage_bits(chunk, years):
    assert BLOCKS == 1 << HALVINGS and SLOTS <= 2 * SUBLANES
    count = years.bit_length() - 1
    assert years == 1 << count and count > HALVINGS
    return [tuple(1 << b for b in pair) for pair in ORDERS[chunk]] + [(1 << b, 1 << b) for b in range(4, count)]


def block_of(chunk):
    year, core = lax.axis_index("year"), lax.rem(lax.axis_index("space"), 2)
    pairs = stage_bits(chunk, lax.axis_size("year"))[:HALVINGS]
    high, low = [jnp.where(core == 0, year // a % 2, year // b % 2) for a, b in pairs]
    return [[2 * p + r for r in (1 - low, low)] for p in (1 - high, high)]


def place(day):
    chunk = sum((day >= c * SLOTS).astype(jnp.int32) for c in range(1, CHUNKS))
    return chunk, day - chunk * SLOTS


def stats_kernel(day_in, tally_in, x_in, *refs):
    outs, (x_ref, day_ref, tally_ref, hours, even, odd, arrived, listed) = refs[: 2 * CHUNKS], refs[2 * CHUNKS :]
    tiles, rows = x_in.shape[0], x_in.shape[1] // BLOCKS
    piece = tiles // PIECES
    height = rows // SUBLANES
    lists = [pltpu.make_async_copy(day_in, day_ref, listed.at[0]), pltpu.make_async_copy(tally_in, tally_ref, listed.at[1])]
    copies = []
    for p in range(PIECES):
        at = pl.ds(p * piece, piece)
        copies.append(pltpu.make_async_copy(x_in.at[at], x_ref.at[at], arrived.at[p]))
    for copy in lists + copies:
        copy.start()
    for i in range(CHUNKS * BLOCKS):
        at = i * TILES
        for totals in (even, odd):
            totals[at : at + HIGH] = jnp.zeros((HIGH, height, LANES), jnp.float32)
            totals[at + HIGH : at + LOW] = jnp.full((SLOTS, height, LANES), -jnp.inf, jnp.float32)
            totals[at + LOW : at + TILES] = jnp.full((SLOTS, height, LANES), jnp.inf, jnp.float32)
    for d in range(CHUNKS * SLOTS):
        hours[d] = 0
    for copy in lists:
        copy.wait()

    def tile(t, carry):
        for k in range(SUBLANES):
            step, totals = t * SUBLANES + k, odd if k % 2 else even
            day, tally = day_ref[step], tally_ref[step]
            chunk, index = place(day)
            base = chunk * (BLOCKS * TILES) + index
            hours[day] += tally
            tally = tally.astype(jnp.float32)
            x = [x_ref[t, pl.ds(b * rows + k, height, stride=SUBLANES), :] for b in range(BLOCKS)]
            at = [[base + b * TILES + kind for kind in (0, HIGH, LOW)] for b in range(BLOCKS)]
            old = [[totals[i] for i in a] for a in at]
            new = [[o[0] + tally * v, jnp.maximum(o[1], v), jnp.minimum(o[2], v)] for o, v in zip(old, x)]
            for a, n in zip(at, new):
                for i, v in zip(a, n):
                    totals[i] = v
        return carry

    for p in range(PIECES):
        copies[p].wait()
        lax.fori_loop(p * piece, (p + 1) * piece, tile, 0)
    left = lax.broadcasted_iota(jnp.int32, (1, LANES), 1) < LANES // 2
    for c in range(CHUNKS):
        blocks = block_of(c)
        pairs = []
        for k in range(SUBLANES):
            pairs.append([hours[c * SLOTS + min(i, SLOTS - 1)].astype(jnp.float32) for i in (k, k + SUBLANES)])
        for half in range(2):
            for slot in range(2):
                out, start = outs[2 * c + half].at[slot], (c * BLOCKS + blocks[half][slot]) * TILES
                for a, b, join in KINDS:
                    at = pl.ds(start + a, b - a)
                    out[a:b] = join(even[at], odd[at])
                for k, pair in enumerate(pairs):
                    out[HOURS, k : k + 1, :] = jnp.where(left, *pair)


def stats(day, tally, x):
    tiles, rows = x.shape[0], x.shape[1] // BLOCKS
    height = rows // SUBLANES
    shapes = (vmem(2, TILES, height, LANES),) * (2 * CHUNKS) + (vmem(*x.shape),)
    return local_call(
        stats_kernel,
        "stats",
        shapes,
        day, tally, x,
        in_specs=[HBM] * 3,
        out_specs=(VMEM,) * len(shapes),
        scratch_shapes=[
            pltpu.SMEM(day.shape, jnp.int32),
            pltpu.SMEM(day.shape, jnp.int32),
            pltpu.SMEM((CHUNKS * SLOTS,), jnp.int32),
            vmem(CHUNKS * BLOCKS * TILES, height, LANES),
            vmem(CHUNKS * BLOCKS * TILES, height, LANES),
            pltpu.SemaphoreType.DMA((PIECES,)),
            pltpu.SemaphoreType.DMA((2,)),
        ],
        vmem=8 << 20,
    )


def merge_kernel(got_ref, own_ref, *outs):
    for a, b, join in KINDS:
        for i, out in enumerate(outs):
            got, own = (got_ref.at[i], own_ref.at[i]) if len(outs) > 1 else (got_ref, own_ref)
            out[a:b] = join(got[a:b], own[a:b])


def table_kernel(got, own, table):
    hours = got[HOURS] + own[HOURS]
    left = lax.broadcasted_iota(jnp.int32, hours.shape, 1) < LANES // 2
    other = pltpu.roll(hours, LANES // 2, axis=1)
    hours = jnp.concatenate([jnp.where(left, hours, other), jnp.where(left, other, hours)])
    for i in range(SLOTS):
        total = got[i] + own[i]
        table[i] = total / jnp.broadcast_to(hours[i : i + 1], total.shape)
        high = jnp.maximum(got[HIGH + i], own[HIGH + i])
        low = jnp.minimum(got[LOW + i], own[LOW + i])
        table[SLOTS + i] = 4.0 / (high - low + 1.0)


def join_kernel(got_ref, own_ref, out_ref):
    out_ref[0] = got_ref[...]
    out_ref[1] = own_ref[...]


def depart_kernel(day_in, x_ref, w_ref, *refs):
    tables, refs = refs[: 2 * CHUNKS], refs[2 * CHUNKS :]
    last_ref, sums_ref, whole_ref, table, ready, squares, left, day_ref, listed = refs
    days = pltpu.make_async_copy(day_in, day_ref, listed)
    days.start()
    tiles, rows = x_ref.shape[0], x_ref.shape[1] // BLOCKS
    piece = tiles // PIECES
    height = rows // SUBLANES
    for c in range(CHUNKS):
        blocks = block_of(c)
        for half in range(2):
            for slot in range(2):
                start = (c * BLOCKS + blocks[half][slot]) * 2 * SLOTS
                table[pl.ds(start, 2 * SLOTS)] = tables[2 * c + half][slot]
    days.wait()
    weights = [w_ref[b * height : (b + 1) * height, :] for b in range(BLOCKS)]

    def tile(first, out_ref, t, carry):
        for k in range(0, SUBLANES, TOGETHER):
            loaded = []
            for j in range(k, k + TOGETHER):
                chunk, index = place(day_ref[t * SUBLANES + j])
                base = chunk * (BLOCKS * 2 * SLOTS) + index
                for b in range(BLOCKS):
                    x = x_ref[t, pl.ds(b * rows + j, height, stride=SUBLANES), :]
                    loaded.append((x, table[base + b * 2 * SLOTS], table[base + (b * 2 + 1) * SLOTS]))
            for j in range(k, k + TOGETHER):
                total = None
                for b in range(BLOCKS):
                    x, mean, scale = loaded[(j - k) * BLOCKS + b]
                    departure = (x - mean) * scale
                    out_ref[t - first, pl.ds(b * rows + j, height, stride=SUBLANES), :] = departure
                    square = weights[b] * departure * departure
                    total = square if total is None else total + square
                squares[pl.ds(pl.multiple_of((t * SUBLANES + j) * height, height), height), :] = total
        return carry

    copies = []
    for p in range(PIECES):
        first, late = p * piece, p >= PIECES - LATE
        before = (PIECES - LATE) * piece if late else 0
        lax.fori_loop(first, first + piece, functools.partial(tile, before, last_ref if late else ready), 0)
        if not late:
            at = pl.ds(first, piece)
            copies.append(pltpu.make_async_copy(ready.at[at], whole_ref.at[at], left.at[p]))
            copies[-1].start()
    sums = []
    for t in range(tiles):
        start = t * SUBLANES * height
        total = squares[pl.ds(start, SUBLANES, stride=height), :]
        for j in range(1, height):
            total += squares[pl.ds(start + j, SUBLANES, stride=height), :]
        sums.append(total)
    by_step = jnp.sum(jnp.concatenate(sums).T, axis=0, keepdims=True)
    sums_ref[0:1, :] = by_step
    sums_ref[1:2, :] = jnp.full(by_step.shape, jnp.sum(w_ref[...]), jnp.float32)
    sums_ref[2:, :] = jnp.zeros((SUBLANES - 2, by_step.shape[1]), jnp.float32)
    for copy in copies:
        copy.wait()


def depart(day, x, w, tables):
    tiles, rows = x.shape[0], x.shape[1] // BLOCKS
    height, late, steps = rows // SUBLANES, tiles // PIECES * LATE, tiles * SUBLANES
    inputs = [day, x, w, *tables]
    return local_call(
        depart_kernel,
        "depart",
        (vmem(late, *x.shape[1:]), vmem(SUBLANES, steps), pltpu.HBM(x.shape, jnp.float32)),
        *inputs,
        in_specs=[VMEM] * len(inputs),
        out_specs=(VMEM, VMEM, HBM),
        scratch_shapes=[
            vmem(CHUNKS * BLOCKS * 2 * SLOTS, height, LANES),
            vmem(tiles - late, *x.shape[1:]),
            vmem(steps * height, LANES),
            pltpu.SemaphoreType.DMA((PIECES - LATE,)),
            pltpu.SMEM(day.shape, jnp.int32),
            pltpu.SemaphoreType.DMA,
        ],
        vmem=8 << 20,
    )


def emit_kernel(part_ref, before_ref, out_ref, left):
    piece, tiles = part_ref.shape[0], out_ref.shape[0]
    copies = []
    for i in range(piece):
        copies.append(pltpu.make_async_copy(part_ref.at[i], out_ref.at[tiles - piece + i], left.at[i]))
        copies[-1].start()
    for copy in copies:
        copy.wait()


def emit(part, out):
    return local_call(
        emit_kernel,
        "emit",
        pltpu.HBM(out.shape, jnp.float32),
        part, out,
        in_specs=[VMEM, HBM],
        out_specs=HBM,
        scratch_shapes=[pltpu.SemaphoreType.DMA((part.shape[0],))],
        input_output_aliases={1: 0},
    )


def exchange(x, pair, name):
    years, spaces = lax.axis_size("year"), lax.axis_size("space")
    partners = [(y * spaces + s, (y ^ pair[s % 2]) * spaces + s) for y in range(years) for s in range(spaces)]
    with jax.named_scope(name):
        return lax.ppermute(pltpu.with_memory_space_constraint(x, pltpu.VMEM), AXES, partners)


def day_tables(chunk, send, keep):
    pairs = stage_bits(chunk, lax.axis_size("year"))
    for stage, pair in enumerate(pairs):
        got = exchange(send if stage < HALVINGS else keep, pair, f"send_{chunk}_{stage}")
        yield
        name = f"merge_{chunk}_{stage}"
        if stage < HALVINGS - 1:
            half = vmem(*got.shape[1:])
            send, keep = local_call(merge_kernel, name, (half, half), got, keep, out_specs=(VMEM, VMEM))
        elif stage < len(pairs) - 1:
            keep = local_call(merge_kernel, name, vmem(*got.shape), got, keep, out_specs=VMEM)
    table = local_call(table_kernel, name, vmem(2 * SLOTS, *got.shape[1:]), got, keep, out_specs=VMEM)
    for stage in reversed(range(HALVINGS)):
        number = len(pairs) + HALVINGS - 1 - stage
        got = exchange(table, pairs[stage], f"send_{chunk}_{number}")
        yield
        if stage > 0:
            table = local_call(join_kernel, f"merge_{chunk}_{number}", vmem(2, *got.shape), got, table, out_specs=VMEM)
    yield got, table


def on_device(thermal_reading, yearday_position, usable_observation_tally, location_surface_factor):
    steps, cells = thermal_reading.shape
    tiles, columns = steps // SUBLANES, cells // LANES
    x = thermal_reading.reshape(tiles, SUBLANES, columns, LANES).transpose(0, 2, 1, 3)
    x = x.reshape(tiles, columns * SUBLANES, LANES)
    w = location_surface_factor.reshape(columns, LANES)
    *halves, x = stats(yearday_position, usable_observation_tally, x)
    chunks = [day_tables(c, *halves[2 * c : 2 * c + 2]) for c in range(CHUNKS)]
    results = [None] * CHUNKS
    while not all(results):
        for c in range(CHUNKS):
            results[c] = next(chunks[c])
    part, sums, out = depart(yearday_position, x, w, [table for pair in results for table in pair])
    out = emit(part, out)
    if lax.axis_size("space") == 2:
        sums += lax.ppermute(sums, "space", [(0, 1), (1, 0)])
    else:
        sums = lax.psum(sums, "space")
    out = out.reshape(tiles, columns, SUBLANES, LANES).transpose(0, 2, 1, 3).reshape(steps, cells)
    return out, sums[0] / sums[1]


def solution(mesh):
    return jax.shard_map(
        on_device,
        mesh=mesh,
        in_specs=(P("year", "space"), P("year"), P("year"), P("space")),
        out_specs=(P("year", "space"), P("year")),
        check_vma=False,
    )
```

```python
import functools
import math

import jax
import jax.numpy as jnp
from jax import lax
from jax.experimental import pallas as pl
from jax.experimental.pallas import tpu as pltpu
from jax.sharding import PartitionSpec as P

DAYS = 30
SUBLANES, LANES = 8, 128
CHUNKS = 3
SLOTS = -(-DAYS // CHUNKS)
BLOCKS = 4
HALVINGS = 2
HOURS, HIGH, LOW, TILES = SLOTS, SLOTS + 1, 2 * SLOTS + 1, 3 * SLOTS + 1
KINDS = (0, HIGH, jnp.add), (HIGH, LOW, jnp.maximum), (LOW, TILES, jnp.minimum)
ORDERS = (((2, 1), (0, 3), (1, 2), (3, 0)), ((0, 1), (2, 3), (3, 0), (1, 2)), ((2, 1), (0, 3), (3, 2), (1, 0)))
AXES = ("year", "space")
PIECES = 8
LATE = 4
TOGETHER = 2

VMEM = pl.BlockSpec(memory_space=pltpu.VMEM)
SMEM = pl.BlockSpec(memory_space=pltpu.SMEM)
HBM = pl.BlockSpec(memory_space=pltpu.HBM)


def local_call(kernel, name, out_shape, *inputs, **options):
    specs = options.pop("in_specs", [VMEM] * len(inputs))
    spaces = {id(VMEM): pltpu.VMEM, id(HBM): pltpu.HBM}
    inputs = [pltpu.with_memory_space_constraint(a, spaces[id(s)]) if id(s) in spaces else a for a, s in zip(inputs, specs)]
    limit = pltpu.CompilerParams(vmem_limit_bytes=options.pop("vmem", 1 << 20))
    return pl.pallas_call(kernel, in_specs=specs, out_shape=out_shape, name=name, compiler_params=limit, **options)(*inputs)


def vmem(*shape):
    return pltpu.VMEM(shape, jnp.float32)


def stage_bits(chunk, years):
    assert BLOCKS == 1 << HALVINGS and SLOTS <= 2 * SUBLANES
    count = years.bit_length() - 1
    assert years == 1 << count and count > HALVINGS
    return [tuple(1 << b for b in pair) for pair in ORDERS[chunk]] + [(1 << b, 1 << b) for b in range(4, count)]


def block_of(chunk):
    year, core = lax.axis_index("year"), lax.rem(lax.axis_index("space"), 2)
    pairs = stage_bits(chunk, lax.axis_size("year"))[:HALVINGS]
    high, low = [jnp.where(core == 0, year // a % 2, year // b % 2) for a, b in pairs]
    return [[2 * p + r for r in (1 - low, low)] for p in (1 - high, high)]


def place(day):
    chunk = sum((day >= c * SLOTS).astype(jnp.int32) for c in range(1, CHUNKS))
    return chunk, day - chunk * SLOTS


def stats_kernel(day_in, tally_in, x_in, *refs):
    outs, (x_ref, day_ref, tally_ref, hours, even, odd, arrived, listed) = refs[: 2 * CHUNKS], refs[2 * CHUNKS :]
    tiles, rows = x_in.shape[0], x_in.shape[1] // BLOCKS
    piece = tiles // PIECES
    height = rows // SUBLANES
    lists = [pltpu.make_async_copy(day_in, day_ref, listed.at[0]), pltpu.make_async_copy(tally_in, tally_ref, listed.at[1])]
    copies = []
    for p in range(PIECES):
        at = pl.ds(p * piece, piece)
        copies.append(pltpu.make_async_copy(x_in.at[at], x_ref.at[at], arrived.at[p]))
    for copy in lists + copies:
        copy.start()
    for i in range(CHUNKS * BLOCKS):
        at = i * TILES
        for totals in (even, odd):
            totals[at : at + HIGH] = jnp.zeros((HIGH, height, LANES), jnp.float32)
            totals[at + HIGH : at + LOW] = jnp.full((SLOTS, height, LANES), -jnp.inf, jnp.float32)
            totals[at + LOW : at + TILES] = jnp.full((SLOTS, height, LANES), jnp.inf, jnp.float32)
    for d in range(CHUNKS * SLOTS):
        hours[d] = 0
    for copy in lists:
        copy.wait()

    def tile(t, carry):
        for k in range(SUBLANES):
            step, totals = t * SUBLANES + k, odd if k % 2 else even
            day, tally = day_ref[step], tally_ref[step]
            chunk, index = place(day)
            base = chunk * (BLOCKS * TILES) + index
            hours[day] += tally
            tally = tally.astype(jnp.float32)
            x = [x_ref[t, pl.ds(b * rows + k, height, stride=SUBLANES), :] for b in range(BLOCKS)]
            at = [[base + b * TILES + kind for kind in (0, HIGH, LOW)] for b in range(BLOCKS)]
            old = [[totals[i] for i in a] for a in at]
            new = [[o[0] + tally * v, jnp.maximum(o[1], v), jnp.minimum(o[2], v)] for o, v in zip(old, x)]
            for a, n in zip(at, new):
                for i, v in zip(a, n):
                    totals[i] = v
        return carry

    for p in range(PIECES):
        copies[p].wait()
        lax.fori_loop(p * piece, (p + 1) * piece, tile, 0)
    left = lax.broadcasted_iota(jnp.int32, (1, LANES), 1) < LANES // 2
    for c in range(CHUNKS):
        blocks = block_of(c)
        pairs = []
        for k in range(SUBLANES):
            pairs.append([hours[c * SLOTS + min(i, SLOTS - 1)].astype(jnp.float32) for i in (k, k + SUBLANES)])
        for half in range(2):
            for slot in range(2):
                out, start = outs[2 * c + half].at[slot], (c * BLOCKS + blocks[half][slot]) * TILES
                for a, b, join in KINDS:
                    at = pl.ds(start + a, b - a)
                    out[a:b] = join(even[at], odd[at])
                for k, pair in enumerate(pairs):
                    out[HOURS, k : k + 1, :] = jnp.where(left, *pair)


def stats(day, tally, x):
    tiles, rows = x.shape[0], x.shape[1] // BLOCKS
    height = rows // SUBLANES
    shapes = (vmem(2, TILES, height, LANES),) * (2 * CHUNKS) + (vmem(*x.shape),)
    return local_call(
        stats_kernel,
        "stats",
        shapes,
        day, tally, x,
        in_specs=[HBM] * 3,
        out_specs=(VMEM,) * len(shapes),
        scratch_shapes=[
            pltpu.SMEM(day.shape, jnp.int32),
            pltpu.SMEM(day.shape, jnp.int32),
            pltpu.SMEM((CHUNKS * SLOTS,), jnp.int32),
            vmem(CHUNKS * BLOCKS * TILES, height, LANES),
            vmem(CHUNKS * BLOCKS * TILES, height, LANES),
            pltpu.SemaphoreType.DMA((PIECES,)),
            pltpu.SemaphoreType.DMA((2,)),
        ],
        vmem=8 << 20,
    )


def merge_kernel(got_ref, own_ref, *outs):
    for a, b, join in KINDS:
        for i, out in enumerate(outs):
            got, own = (got_ref.at[i], own_ref.at[i]) if len(outs) > 1 else (got_ref, own_ref)
            out[a:b] = join(got[a:b], own[a:b])


def table_kernel(got, own, table):
    hours = got[HOURS] + own[HOURS]
    left = lax.broadcasted_iota(jnp.int32, hours.shape, 1) < LANES // 2
    other = pltpu.roll(hours, LANES // 2, axis=1)
    hours = jnp.concatenate([jnp.where(left, hours, other), jnp.where(left, other, hours)])
    for i in range(SLOTS):
        total = got[i] + own[i]
        table[i] = total / jnp.broadcast_to(hours[i : i + 1], total.shape)
        high = jnp.maximum(got[HIGH + i], own[HIGH + i])
        low = jnp.minimum(got[LOW + i], own[LOW + i])
        table[SLOTS + i] = 4.0 / (high - low + 1.0)


def join_kernel(got_ref, own_ref, out_ref):
    out_ref[0] = got_ref[...]
    out_ref[1] = own_ref[...]


def depart_kernel(day_in, x_ref, w_ref, *refs):
    tables, refs = refs[: 2 * CHUNKS], refs[2 * CHUNKS :]
    last_ref, sums_ref, whole_ref, table, ready, squares, left, day_ref, listed = refs
    days = pltpu.make_async_copy(day_in, day_ref, listed)
    days.start()
    tiles, rows = x_ref.shape[0], x_ref.shape[1] // BLOCKS
    piece = tiles // PIECES
    height = rows // SUBLANES
    for c in range(CHUNKS):
        blocks = block_of(c)
        for half in range(2):
            for slot in range(2):
                start = (c * BLOCKS + blocks[half][slot]) * 2 * SLOTS
                table[pl.ds(start, 2 * SLOTS)] = tables[2 * c + half][slot]
    days.wait()
    weights = [w_ref[b * height : (b + 1) * height, :] for b in range(BLOCKS)]

    def tile(first, out_ref, t, carry):
        for k in range(0, SUBLANES, TOGETHER):
            loaded = []
            for j in range(k, k + TOGETHER):
                chunk, index = place(day_ref[t * SUBLANES + j])
                base = chunk * (BLOCKS * 2 * SLOTS) + index
                for b in range(BLOCKS):
                    x = x_ref[t, pl.ds(b * rows + j, height, stride=SUBLANES), :]
                    loaded.append((x, table[base + b * 2 * SLOTS], table[base + (b * 2 + 1) * SLOTS]))
            for j in range(k, k + TOGETHER):
                total = None
                for b in range(BLOCKS):
                    x, mean, scale = loaded[(j - k) * BLOCKS + b]
                    departure = (x - mean) * scale
                    out_ref[t - first, pl.ds(b * rows + j, height, stride=SUBLANES), :] = departure
                    square = weights[b] * departure * departure
                    total = square if total is None else total + square
                squares[pl.ds(pl.multiple_of((t * SUBLANES + j) * height, height), height), :] = total
        return carry

    copies = []
    for p in range(PIECES):
        first, late = p * piece, p >= PIECES - LATE
        before = (PIECES - LATE) * piece if late else 0
        lax.fori_loop(first, first + piece, functools.partial(tile, before, last_ref if late else ready), 0)
        if not late:
            at = pl.ds(first, piece)
            copies.append(pltpu.make_async_copy(ready.at[at], whole_ref.at[at], left.at[p]))
            copies[-1].start()
    sums = []
    for t in range(tiles):
        start = t * SUBLANES * height
        total = squares[pl.ds(start, SUBLANES, stride=height), :]
        for j in range(1, height):
            total += squares[pl.ds(start + j, SUBLANES, stride=height), :]
        sums.append(total)
    by_step = jnp.sum(jnp.concatenate(sums).T, axis=0, keepdims=True)
    sums_ref[0:1, :] = by_step
    sums_ref[1:2, :] = jnp.full(by_step.shape, jnp.sum(w_ref[...]), jnp.float32)
    sums_ref[2:, :] = jnp.zeros((SUBLANES - 2, by_step.shape[1]), jnp.float32)
    for copy in copies:
        copy.wait()


def depart(day, x, w, tables):
    tiles, rows = x.shape[0], x.shape[1] // BLOCKS
    height, late, steps = rows // SUBLANES, tiles // PIECES * LATE, tiles * SUBLANES
    inputs = [day, x, w, *tables]
    return local_call(
        depart_kernel,
        "depart",
        (vmem(late, *x.shape[1:]), vmem(SUBLANES, steps), pltpu.HBM(x.shape, jnp.float32)),
        *inputs,
        in_specs=[VMEM] * len(inputs),
        out_specs=(VMEM, VMEM, HBM),
        scratch_shapes=[
            vmem(CHUNKS * BLOCKS * 2 * SLOTS, height, LANES),
            vmem(tiles - late, *x.shape[1:]),
            vmem(steps * height, LANES),
            pltpu.SemaphoreType.DMA((PIECES - LATE,)),
            pltpu.SMEM(day.shape, jnp.int32),
            pltpu.SemaphoreType.DMA,
        ],
        vmem=8 << 20,
    )


def emit_kernel(part_ref, before_ref, out_ref, left):
    piece, tiles = part_ref.shape[0], out_ref.shape[0]
    copies = []
    for i in range(piece):
        copies.append(pltpu.make_async_copy(part_ref.at[i], out_ref.at[tiles - piece + i], left.at[i]))
        copies[-1].start()
    for copy in copies:
        copy.wait()


def emit(part, out):
    return local_call(
        emit_kernel,
        "emit",
        pltpu.HBM(out.shape, jnp.float32),
        part, out,
        in_specs=[VMEM, HBM],
        out_specs=HBM,
        scratch_shapes=[pltpu.SemaphoreType.DMA((part.shape[0],))],
        input_output_aliases={1: 0},
    )


def exchange(x, pair, name):
    years, spaces = lax.axis_size("year"), lax.axis_size("space")
    partners = [(y * spaces + s, (y ^ pair[s % 2]) * spaces + s) for y in range(years) for s in range(spaces)]
    with jax.named_scope(name):
        return lax.ppermute(pltpu.with_memory_space_constraint(x, pltpu.VMEM), AXES, partners)


def day_tables(chunk, send, keep):
    pairs = stage_bits(chunk, lax.axis_size("year"))
    for stage, pair in enumerate(pairs):
        got = exchange(send if stage < HALVINGS else keep, pair, f"send_{chunk}_{stage}")
        yield
        name = f"merge_{chunk}_{stage}"
        if stage < HALVINGS - 1:
            half = vmem(*got.shape[1:])
            send, keep = local_call(merge_kernel, name, (half, half), got, keep, out_specs=(VMEM, VMEM))
        elif stage < len(pairs) - 1:
            keep = local_call(merge_kernel, name, vmem(*got.shape), got, keep, out_specs=VMEM)
    table = local_call(table_kernel, name, vmem(2 * SLOTS, *got.shape[1:]), got, keep, out_specs=VMEM)
    for stage in reversed(range(HALVINGS)):
        number = len(pairs) + HALVINGS - 1 - stage
        got = exchange(table, pairs[stage], f"send_{chunk}_{number}")
        yield
        if stage > 0:
            table = local_call(join_kernel, f"merge_{chunk}_{number}", vmem(2, *got.shape), got, table, out_specs=VMEM)
    yield got, table


def on_device(thermal_reading, yearday_position, usable_observation_tally, location_surface_factor):
    steps, cells = thermal_reading.shape
    tiles, columns = steps // SUBLANES, cells // LANES
    x = thermal_reading.reshape(tiles, SUBLANES, columns, LANES).transpose(0, 2, 1, 3)
    x = x.reshape(tiles, columns * SUBLANES, LANES)
    w = location_surface_factor.reshape(columns, LANES)
    *halves, x = stats(yearday_position, usable_observation_tally, x)
    chunks = [day_tables(c, *halves[2 * c : 2 * c + 2]) for c in range(CHUNKS)]
    results = [None] * CHUNKS
    while not all(results):
        for c in range(CHUNKS):
            results[c] = next(chunks[c])
    part, sums, out = depart(yearday_position, x, w, [table for pair in results for table in pair])
    out = emit(part, out)
    if lax.axis_size("space") == 2:
        sums += lax.ppermute(sums, "space", [(0, 1), (1, 0)])
    else:
        sums = lax.psum(sums, "space")
    out = out.reshape(tiles, columns, SUBLANES, LANES).transpose(0, 2, 1, 3).reshape(steps, cells)
    return out, sums[0] / sums[1]


def solution(mesh):
    return jax.shard_map(
        on_device,
        mesh=mesh,
        in_specs=(P("year", "space"), P("year"), P("year"), P("space")),
        out_specs=(P("year", "space"), P("year")),
        check_vma=False,
    )
```
